32 devices in a mesh: dp: 1 (over z), cp: 32 (over y, x, core).
Axes of the slice: x: 4, y: 4, z: 1, core: 2. Of those that a mesh axis runs over, the one named last changes fastest.
The devices are a block of a 4x4x8 slice.
Arguments:
- hidden: bfloat16 [1, 8192, 2560], P('dp', 'cp')
- grad_out: bfloat16 [1, 8192, 2560], P('dp', 'cp')
- norm_gain: float32 [2, 2560], replicated
- w_qkv: bfloat16 [2, 2560, 4096], replicated
- b_qkv: float32 [2, 4096], replicated
- w_out: bfloat16 [2, 2048, 2560], replicated
- b_out: float32 [2, 2560], replicated
- attn_sinks: float32 [2, 8], replicated
Outputs:
- output 1: bfloat16 [1, 8192, 2560], P('dp', 'cp')
- output 2: bfloat16 [1, 8192, 2560], P('dp', 'cp')
- output 3: float32 [32, 2, 2560], P(('dp', 'cp'))
- output 4: float32 [32, 2, 4096], P(('dp', 'cp'))
- output 5: float32 [32, 2, 2560], P(('dp', 'cp'))
- output 6: float32 [32, 2, 8], P(('dp', 'cp'))
All inputs are finite; a program needn't handle non-finite values.
Results may differ from the reference program's by a relative error of at most 0.0170665.
Values are sent between devices in bfloat16 or wider.
A program may use at most 768 MiB of HBM per device.

```python
import jax
import jax.numpy as jnp
import math
from jax import lax

BATCH = 1
SEQ = 8192
CHUNKS = 32
D = 2560
HEADS = 8
KV_HEADS = 4
HEAD = 256
WINDOW = 128
SEQ_DEV = SEQ // CHUNKS
GROUP = HEADS // KV_HEADS
Q_WIDTH = HEADS * HEAD
K_WIDTH = KV_HEADS * HEAD
QKV = Q_WIDTH + 2 * K_WIDTH
SCALE = HEAD ** -0.5
EPSILON = 1e-5
ROPE_THETA = 150000.0
YARN_FACTOR = 32.0
YARN_CONTEXT = 4096.0
YARN_ALPHA = 1.0
YARN_BETA = 32.0


def rope_tables(positions):
    half_dim = HEAD // 2
    freq_steps = jnp.arange(half_dim, dtype=jnp.float32)
    freq_base = ROPE_THETA ** (freq_steps * 2.0 / HEAD)
    concentration = 0.1 * math.log(YARN_FACTOR) + 1.0
    low_edge = half_dim * math.log(YARN_CONTEXT / (YARN_BETA * 2.0 * math.pi)) / math.log(ROPE_THETA)
    high_edge = half_dim * math.log(YARN_CONTEXT / (YARN_ALPHA * 2.0 * math.pi)) / math.log(ROPE_THETA)
    ramp_pos = jnp.clip((freq_steps - low_edge) / (high_edge - low_edge), 0.0, 1.0)
    inv_freq = (1.0 - ramp_pos) / freq_base + ramp_pos / (YARN_FACTOR * freq_base)
    angles = positions.astype(jnp.float32)[:, None] * inv_freq[None, :]
    return jnp.cos(angles) * concentration, jnp.sin(angles) * concentration


def rotate_half(tensor, cos_tab, sin_tab):
    half_dim = tensor.shape[-1] // 2
    first_half = tensor[..., :half_dim]
    second_half = tensor[..., half_dim:]
    return jnp.concatenate([first_half * cos_tab - second_half * sin_tab, second_half * cos_tab + first_half * sin_tab], axis=-1)


def attention_layer(hidden, gain_c, w_in, bias_c, w_proj, bout_c, sink_c, cos_tab, sin_tab, window_on):
    hid_f = hidden.astype(jnp.float32)
    inv_rms = lax.rsqrt(jnp.mean(hid_f * hid_f, axis=-1, keepdims=True) + EPSILON)
    normed = ((hid_f * inv_rms).reshape(BATCH, CHUNKS, SEQ_DEV, D) * gain_c[None, :, None, :]).reshape(BATCH, SEQ, D).astype(jnp.bfloat16)
    projected = jnp.dot(normed, w_in, preferred_element_type=jnp.float32)
    projected = (projected.reshape(BATCH, CHUNKS, SEQ_DEV, QKV) + bias_c[None, :, None, :]).reshape(BATCH, SEQ, QKV)
    query_rows = rotate_half(projected[..., :Q_WIDTH].reshape(BATCH, SEQ, KV_HEADS, GROUP, HEAD), cos_tab[:, None, None, :], sin_tab[:, None, None, :]).astype(jnp.bfloat16)
    key_rows = rotate_half(projected[..., Q_WIDTH:Q_WIDTH + K_WIDTH].reshape(BATCH, SEQ, KV_HEADS, HEAD), cos_tab[:, None, :], sin_tab[:, None, :]).astype(jnp.bfloat16)
    value_rows = projected[..., Q_WIDTH + K_WIDTH:].reshape(BATCH, SEQ, KV_HEADS, HEAD).astype(jnp.bfloat16)
    positions = jnp.arange(SEQ)
    query_blocks = jnp.moveaxis(query_rows.reshape(BATCH, CHUNKS, SEQ_DEV, KV_HEADS, GROUP, HEAD), 1, 0)
    row_blocks = positions.reshape(CHUNKS, SEQ_DEV)
    sink_blocks = sink_c.reshape(CHUNKS, KV_HEADS, GROUP)
    keys_f = key_rows.astype(jnp.float32)
    values_f = value_rows.astype(jnp.float32)

    def one_block(block_args):
        query_blk, row_pos, sink_row = block_args
        scores = SCALE * jnp.einsum('bqkgd,bskd->bkgqs', query_blk.astype(jnp.float32), keys_f)
        allowed = positions[None, :] <= row_pos[:, None]
        if window_on:
            allowed = allowed & (positions[None, :] >= row_pos[:, None] - WINDOW)
        scores = jnp.where(allowed, scores, -jnp.inf)
        sink_grid = sink_row[None, :, :, None]
        row_peak = lax.stop_gradient(jnp.maximum(jnp.max(scores, axis=-1), sink_grid))
        exp_scores = jnp.exp(scores - row_peak[..., None])
        denominator = jnp.sum(exp_scores, axis=-1) + jnp.exp(sink_grid - row_peak)
        prob_bf = (exp_scores / denominator[..., None]).astype(jnp.bfloat16)
        return jnp.einsum('bkgqs,bskd->bqkgd', prob_bf.astype(jnp.float32), values_f).astype(jnp.bfloat16)

    attn_out = lax.map(jax.checkpoint(one_block), (query_blocks, row_blocks, sink_blocks))
    attn_out = jnp.moveaxis(attn_out, 0, 1).reshape(BATCH, SEQ, Q_WIDTH)
    out_proj = jnp.dot(attn_out, w_proj, preferred_element_type=jnp.float32)
    out_proj = (out_proj.reshape(BATCH, CHUNKS, SEQ_DEV, D) + bout_c[None, :, None, :]).reshape(BATCH, SEQ, D)
    return (hid_f + out_proj).astype(jnp.bfloat16)


def setup_inputs(seed: int = 0, part: int = 0) -> dict:
    part_key = jax.random.fold_in(jax.random.key(seed), part)
    key_hidden, key_grad = jax.random.split(part_key)
    shared = jax.random.split(jax.random.key(seed + 1), 6)
    hidden = jax.random.normal(key_hidden, (BATCH, SEQ, D), jnp.float32).astype(jnp.bfloat16)
    grad_out = jax.random.normal(key_grad, (BATCH, SEQ, D), jnp.float32).astype(jnp.bfloat16)
    norm_gain = 1.0 + 0.3 * jax.random.normal(shared[0], (2, D), jnp.float32)
    w_qkv = (jax.random.normal(shared[1], (2, D, QKV), jnp.float32) * D ** -0.5).astype(jnp.bfloat16)
    b_qkv = 0.3 * jax.random.normal(shared[2], (2, QKV), jnp.float32)
    w_out = (jax.random.normal(shared[3], (2, Q_WIDTH, D), jnp.float32) * Q_WIDTH ** -0.5).astype(jnp.bfloat16)
    b_out = 0.3 * jax.random.normal(shared[4], (2, D), jnp.float32)
    sink_base = jnp.array([math.log(WINDOW + 1.0), math.log(SEQ / 2.0)], jnp.float32)[:, None] + 1.0
    attn_sinks = sink_base + jax.random.normal(shared[5], (2, HEADS), jnp.float32)
    return {'hidden': hidden, 'grad_out': grad_out, 'norm_gain': norm_gain, 'w_qkv': w_qkv, 'b_qkv': b_qkv, 'w_out': w_out, 'b_out': b_out, 'attn_sinks': attn_sinks}


def reference(hidden, grad_out, norm_gain, w_qkv, b_qkv, w_out, b_out, attn_sinks):
    cos_tab, sin_tab = rope_tables(jnp.arange(SEQ))

    def forward(hid_in, gain_t, bias_t, bout_t, sink_t):
        middle = attention_layer(hid_in, gain_t[0], w_qkv[0], bias_t[0], w_out[0], bout_t[0], sink_t[0], cos_tab, sin_tab, True)
        return attention_layer(middle, gain_t[1], w_qkv[1], bias_t[1], w_out[1], bout_t[1], sink_t[1], cos_tab, sin_tab, False)

    def tile_rows(row_table):
        return jnp.broadcast_to(row_table[:, None, :], (2, CHUNKS, row_table.shape[-1]))

    output, pullback = jax.vjp(forward, hidden, tile_rows(norm_gain), tile_rows(b_qkv), tile_rows(b_out), tile_rows(attn_sinks))
    d_hidden, d_gain, d_bias, d_bout, d_sink = pullback(grad_out)
    return output, d_hidden, jnp.swapaxes(d_gain, 0, 1), jnp.swapaxes(d_bias, 0, 1), jnp.swapaxes(d_bout, 0, 1), jnp.swapaxes(d_sink, 0, 1)
```

```python
import functools

import jax
import jax.numpy as jnp
import math
from jax import lax
from jax.experimental import pallas as pl
from jax.experimental.pallas import tpu as pltpu
from jax.sharding import PartitionSpec as P

WINDOW = 128
EPSILON = 1e-5
ROPE_THETA = 150000.0
YARN_FACTOR = 32.0
YARN_CONTEXT = 4096.0
YARN_ALPHA = 1.0
YARN_BETA = 32.0


def rope_tables(positions, head_dim):
    half_dim = head_dim // 2
    freq_steps = jnp.arange(half_dim, dtype=jnp.float32)
    freq_base = ROPE_THETA ** (freq_steps * 2.0 / head_dim)
    concentration = 0.1 * math.log(YARN_FACTOR) + 1.0
    low_edge = half_dim * math.log(YARN_CONTEXT / (YARN_BETA * 2.0 * math.pi)) / math.log(ROPE_THETA)
    high_edge = half_dim * math.log(YARN_CONTEXT / (YARN_ALPHA * 2.0 * math.pi)) / math.log(ROPE_THETA)
    ramp_pos = jnp.clip((freq_steps - low_edge) / (high_edge - low_edge), 0.0, 1.0)
    inv_freq = (1.0 - ramp_pos) / freq_base + ramp_pos / (YARN_FACTOR * freq_base)
    angles = positions.astype(jnp.float32)[:, None] * inv_freq[None, :]
    return jnp.cos(angles) * concentration, jnp.sin(angles) * concentration


def rotate_half(tensor, cos_tab, sin_tab):
    half_dim = tensor.shape[-1] // 2
    first_half = tensor[..., :half_dim]
    second_half = tensor[..., half_dim:]
    return jnp.concatenate([first_half * cos_tab - second_half * sin_tab, second_half * cos_tab + first_half * sin_tab], axis=-1)


def norm_project(hid_f, gain_row, w_in, bias_row, cos_tab, sin_tab, num_heads, kv_heads):
    batch_size, seq_dev = hid_f.shape[0], hid_f.shape[1]
    head_dim = 2 * cos_tab.shape[-1]
    q_width = num_heads * head_dim
    k_width = kv_heads * head_dim
    inv_rms = lax.rsqrt(jnp.mean(hid_f * hid_f, axis=-1, keepdims=True) + EPSILON)
    normed = (hid_f * inv_rms * gain_row).astype(jnp.bfloat16)
    projected = jnp.dot(normed, w_in, preferred_element_type=jnp.float32) + bias_row
    query_rows = rotate_half(projected[..., :q_width].reshape(batch_size, seq_dev, kv_heads, num_heads // kv_heads, head_dim), cos_tab[:, None, None, :], sin_tab[:, None, None, :])
    key_rows = rotate_half(projected[..., q_width:q_width + k_width].reshape(batch_size, seq_dev, kv_heads, head_dim), cos_tab[:, None, :], sin_tab[:, None, :])
    value_rows = projected[..., q_width + k_width:].reshape(batch_size, seq_dev, kv_heads, head_dim)
    return query_rows.astype(jnp.bfloat16), key_rows.astype(jnp.bfloat16), value_rows.astype(jnp.bfloat16), inv_rms


def attend_forward(query_rows, key_rows, value_rows, sink_row, row_pos, key_pos, window_on, logit_scale):
    kv_heads, group_size = query_rows.shape[2], query_rows.shape[3]
    scores = jnp.einsum('bqkgd,bskd->bkgqs', query_rows, key_rows, preferred_element_type=jnp.float32) * logit_scale
    key_mask = (key_pos[None, :] <= row_pos[:, None]) & (key_pos[None, :] >= 0)
    if window_on:
        key_mask = key_mask & (key_pos[None, :] >= row_pos[:, None] - WINDOW)
    scores = jnp.where(key_mask, scores, -jnp.inf)
    sink_grid = sink_row.reshape(kv_heads, group_size)[None, :, :, None]
    row_peak = jnp.maximum(jnp.max(scores, axis=-1), sink_grid)
    exp_scores = jnp.exp(scores - row_peak[..., None])
    sink_exp = jnp.exp(sink_grid - row_peak)
    denominator = jnp.sum(exp_scores, axis=-1) + sink_exp
    prob_f32 = exp_scores / denominator[..., None]
    prob_bf = prob_f32.astype(jnp.bfloat16)
    attn_out = jnp.einsum('bkgqs,bskd->bqkgd', prob_bf, value_rows, preferred_element_type=jnp.float32).astype(jnp.bfloat16)
    return attn_out, prob_f32, prob_bf, sink_exp / denominator


def attend_backward(d_attn, query_rows, key_rows, value_rows, prob_f32, prob_bf, sink_prob, logit_scale):
    d_prob = jnp.einsum('bqkgd,bskd->bkgqs', d_attn, value_rows, preferred_element_type=jnp.float32).astype(jnp.bfloat16).astype(jnp.float32)
    row_delta = jnp.sum(prob_f32 * d_prob, axis=-1)
    d_scores = (prob_f32 * (d_prob - row_delta[..., None])).astype(jnp.bfloat16)
    d_query = (jnp.einsum('bkgqs,bskd->bqkgd', d_scores, key_rows, preferred_element_type=jnp.float32) * logit_scale).astype(jnp.bfloat16)
    d_keys = jnp.einsum('bkgqs,bqkgd->bskd', d_scores, query_rows, preferred_element_type=jnp.float32) * logit_scale
    d_values = jnp.einsum('bkgqs,bqkgd->bskd', prob_bf, d_attn, preferred_element_type=jnp.float32)
    d_sink = -jnp.sum(sink_prob * row_delta, axis=(0, 3)).reshape(-1)
    return d_query, d_keys, d_values, d_sink


def project_backward(d_query, d_keys, d_values, hid_f, inv_rms, gain_row, w_in, cos_tab, sin_tab):
    batch_size, seq_dev = hid_f.shape[0], hid_f.shape[1]
    dq_rot = rotate_half(d_query.astype(jnp.float32), cos_tab[:, None, None, :], -sin_tab[:, None, None, :]).reshape(batch_size, seq_dev, -1)
    dk_rot = rotate_half(d_keys.astype(jnp.float32), cos_tab[:, None, :], -sin_tab[:, None, :]).reshape(batch_size, seq_dev, -1)
    d_proj = jnp.concatenate([dq_rot, dk_rot, d_values.astype(jnp.float32).reshape(batch_size, seq_dev, -1)], axis=-1)
    d_bias = jnp.sum(d_proj, axis=(0, 1))
    d_normed = jnp.einsum('bsq,dq->bsd', d_proj.astype(jnp.bfloat16), w_in, preferred_element_type=jnp.float32).astype(jnp.bfloat16).astype(jnp.float32)
    d_gain = jnp.sum(d_normed * hid_f * inv_rms, axis=(0, 1))
    unit_grad = d_normed * gain_row
    d_hid = inv_rms * unit_grad - hid_f * inv_rms ** 3 * jnp.mean(unit_grad * hid_f, axis=-1, keepdims=True)
    return d_hid, d_gain, d_bias


def dense_out(attn_out, w_proj, bias_row):
    batch_size, seq_dev = attn_out.shape[0], attn_out.shape[1]
    return jnp.dot(attn_out.reshape(batch_size, seq_dev, -1), w_proj, preferred_element_type=jnp.float32) + bias_row


MESH = pl.DeviceIdType.MESH
F32 = jnp.float32
BF16 = jnp.bfloat16


def far_attention_kernel(dims, sink_ref, q_ref, kv_ref, do_ref, o_out, dq_out, dkv_out, dsink_out,
                         q_all, do_all, kv_all, o_acc, dq_acc, m_ref, l_ref, delta_ref,
                         d_acc, o_stage, ds_stage, sib_send, sib_recv, far_send, far_recv, near_send, near_recv,
                         y_ssem, y_rsem, sib_ssem, sib_rsem, near_ssem, near_rsem, relay_ssem, relay_rsem,
                         bsib_ssem, bsib_rsem, bfar_ssem, bfar_rsem, bnear_ssem, bnear_rsem):
    heads, cores, cols, rows, width = dims
    pair = cores * rows
    scale = width ** -0.5
    me = lax.axis_index('cp')
    core = lax.rem(me, cores)
    x = lax.rem(me // cores, cols)
    y = me // (cores * cols)
    sib = lax.rem(core + 1, cores)

    def device(yy, xx, cc):
        return (yy * cols + xx) * cores + cc

    right = lax.rem(x + 1, cols)
    left = lax.rem(x + cols - 1, cols)
    far = lax.rem(x + 2, cols)
    offsets = [(dy, dc) for dy in (1, 3, 2, 0) for dc in range(cores) if (dy, dc) != (0, 0)]

    barrier = pltpu.get_barrier_semaphore()
    partners = [device(lax.rem(y + dy, heads), x, lax.rem(core + dc, cores)) for dy, dc in offsets]
    partners += [device(y, right, core), device(y, left, core)]
    for other in partners:
        pl.semaphore_signal(barrier, inc=1, device_id={'cp': other}, device_id_type=MESH)
    pl.semaphore_wait(barrier, len(partners))

    def remote(src, dst, ssem, rsem, target):
        return pltpu.make_async_remote_copy(src_ref=src, dst_ref=dst, send_sem=ssem, recv_sem=rsem,
                                            device_id={'cp': target}, device_id_type=MESH)

    pending = []

    def exchange(kind, src_of, dst_of):
        copies = {}
        for dy, dc in offsets + [(0, 0)]:
            ty, tc = lax.rem(y + dy, heads), lax.rem(core + dc, cores)
            if (dy, dc) == (0, 0):
                copy = pltpu.make_async_copy(src_of(ty, tc), dst_of(ty, tc), y_rsem.at[kind, dy, dc])
            else:
                copy = remote(src_of(ty, tc), dst_of(ty, tc), y_ssem.at[kind, dy, dc], y_rsem.at[kind, dy, dc], device(ty, x, tc))
                pending.append(copy)
            copy.start()
            copies[dy, dc] = copy
        return copies

    def arrive(copies, key):
        if key == (0, 0):
            copies[key].wait()
        else:
            copies[key].wait_recv()

    def lanes(block, size):
        return pl.ds(pl.multiple_of(block * size, size), size)

    my_rows = lanes(core, rows)
    kv_copies = exchange(0, lambda ty, tc: kv_ref.at[:, lanes(tc * heads + ty, width)],
                         lambda ty, tc: kv_all.at[tc, x, y, my_rows])
    q_copies = exchange(1, lambda ty, tc: q_ref.at[:, lanes(ty * cores + tc, width)],
                        lambda ty, tc: q_all.at[y, my_rows])
    do_copies = exchange(2, lambda ty, tc: do_ref.at[:, lanes(ty * cores + tc, width)],
                         lambda ty, tc: do_all.at[y, my_rows])

    sink = sink_ref[y * cores + core]
    m_ref[...] = jnp.zeros_like(m_ref) + sink
    l_ref[...] = jnp.ones_like(l_ref)
    o_acc[...] = jnp.zeros_like(o_acc)
    dq_acc[...] = jnp.zeros_like(dq_acc)

    order = (0, 1, 3, 2)
    sib_copies = {}
    near_copies = {}
    relay_copies = {}

    def to_sibling(rel, col, dy, piece):
        copy = remote(kv_all.at[core, col, piece], kv_all.at[core, col, piece], sib_ssem.at[rel, dy], sib_rsem.at[rel, dy], device(y, x, sib))
        copy.start()
        pending.append(copy)
        sib_copies[rel, dy] = copy

    def piece_of(dy):
        return lax.rem(y + heads - dy, heads)

    for dy in order:
        for dc in range(cores):
            arrive(kv_copies, (dy, dc))
        piece = piece_of(dy)
        for way, col in ((0, right), (1, left)):
            copy = remote(kv_all.at[core, x, piece], kv_all.at[core, x, piece], near_ssem.at[way, dy], near_rsem.at[way, dy], device(y, col, core))
            copy.start()
            pending.append(copy)
            near_copies[way, dy] = copy
        to_sibling(0, x, dy, piece)

    def relay(dy):
        piece = piece_of(dy)
        near_copies[0, dy].wait_recv()
        if dy in (0, 1):
            copy = remote(kv_all.at[core, left, piece], kv_all.at[core, left, piece], relay_ssem.at[dy], relay_rsem.at[dy], device(y, right, core))
            copy.start()
            pending.append(copy)
            relay_copies[dy] = copy
        to_sibling(3, left, dy, piece)
        near_copies[1, dy].wait_recv()
        if dy in (2, 3):
            copy = remote(kv_all.at[core, right, piece], kv_all.at[core, right, piece], relay_ssem.at[dy], relay_rsem.at[dy], device(y, left, core))
            copy.start()
            pending.append(copy)
            relay_copies[dy] = copy
        to_sibling(1, right, dy, piece)

    def scores(key_blk, query_blk, masked):
        out = lax.dot_general(key_blk, query_blk, (((1,), (1,)), ((), ())), preferred_element_type=F32) * scale
        if masked:
            key_pos = lax.broadcasted_iota(jnp.int32, out.shape, 0)
            query_pos = lax.broadcasted_iota(jnp.int32, out.shape, 1)
            out = jnp.where(key_pos <= query_pos, out, -jnp.inf)
        return out

    def forward_block(col, yk, yq, masked):
        value_blk = kv_all[1, col, yk]
        logits = scores(kv_all[0, col, yk], q_all[yq], masked)
        old_peak = m_ref[yq]
        peak = jnp.maximum(old_peak, jnp.max(logits, axis=0, keepdims=True))
        shrink = jnp.exp(old_peak - peak)
        weight = jnp.exp(logits - peak)
        m_ref[yq] = peak
        l_ref[yq] = l_ref[yq] * shrink + jnp.sum(weight, axis=0, keepdims=True)
        o_acc[yq] = o_acc[yq] * shrink + lax.dot_general(value_blk, weight.astype(BF16), (((0,), (0,)), ((), ())), preferred_element_type=F32)

    def backward_block(rel, col, yk, yq, masked):
        key_blk, value_blk = kv_all[0, col, yk], kv_all[1, col, yk]
        query_blk, grad_blk = q_all[yq], do_all[yq]
        prob = jnp.exp(scores(key_blk, query_blk, masked) - m_ref[yq])
        d_prob = lax.dot_general(value_blk, grad_blk, (((1,), (1,)), ((), ())), preferred_element_type=F32).astype(BF16).astype(F32)
        d_score = (prob * (d_prob - delta_ref[yq])).astype(BF16)
        d_acc[rel, 1, yk] += jnp.dot(prob.astype(BF16), grad_blk, preferred_element_type=F32)
        d_acc[rel, 0, yk] += jnp.dot(d_score, query_blk, preferred_element_type=F32)
        dq_acc[yq] += lax.dot_general(key_blk, d_score, (((0,), (0,)), ((), ())), preferred_element_type=F32)

    def sweep(block, rel, col):
        skip = 1 if rel == 0 else jnp.where(col > x, 1, 0)

        def over_keys(yk, carry):
            if rel == 0:
                block(yk, yk, True)

            def over_queries(yq, inner):
                block(yk, yq, False)
                return inner

            lax.fori_loop(yk + skip, heads, over_queries, 0)
            return carry

        lax.fori_loop(0, heads, over_keys, 0)

    cols_of = {0: x, 1: right, 2: far, 3: left}

    def forward(rel):
        col = cols_of[rel]
        sweep(lambda yk, yq, masked: forward_block(col, yk, yq, masked), rel, col)

    def backward(rel):
        col = cols_of[rel]
        sweep(lambda yk, yq, masked: backward_block(rel, col, yk, yq, masked), rel, col)

    def await_sibling(rel):
        for dy in order:
            sib_copies[rel, dy].wait_recv()

    relay(0)
    relay(1)
    for key in offsets + [(0, 0)]:
        arrive(q_copies, key)
    await_sibling(0)
    forward(0)
    relay(3)
    relay(2)
    d_acc[...] = jnp.zeros_like(d_acc)
    await_sibling(1)
    await_sibling(3)
    forward(1)
    forward(3)
    for dy in order:
        relay_copies[dy].wait_recv()
        to_sibling(2, far, dy, piece_of(dy))
    await_sibling(2)
    forward(2)

    for key in offsets + [(0, 0)]:
        arrive(do_copies, key)

    def finish_forward(yq, carry):
        attn = o_acc[yq] / l_ref[yq]
        lse = m_ref[yq] + jnp.log(l_ref[yq])
        delta = jnp.sum(attn * jnp.transpose(do_all[yq].astype(F32)), axis=0, keepdims=True)
        o_stage[0, yq] = jnp.transpose(attn).astype(BF16)
        m_ref[yq] = lse
        delta_ref[yq] = delta
        contribution = -jnp.exp(sink - lse) * delta
        for part in range(cores):
            total = jnp.sum(contribution[:, part * rows:(part + 1) * rows], axis=1, keepdims=True)
            ds_stage[yq * cores + part] = jnp.zeros(ds_stage.shape[1:], F32) + total
        return carry

    lax.fori_loop(0, heads, finish_forward, 0)

    mine = y * cores + core
    o_copies = exchange(3, lambda ty, tc: o_stage.at[0, ty, lanes(tc, rows)], lambda ty, tc: o_out.at[:, lanes(mine, width)])
    ds_copies = exchange(4, lambda ty, tc: ds_stage.at[ty * cores + tc], lambda ty, tc: dsink_out.at[mine])

    bsib_copies = {}

    def swap_partial(rel):
        sib_send[rel] = d_acc[rel, sib].astype(BF16)
        copy = remote(sib_send.at[rel], sib_recv.at[rel], bsib_ssem.at[rel], bsib_rsem.at[rel], device(y, x, sib))
        copy.start()
        pending.append(copy)
        bsib_copies[rel] = copy

    half = heads // 2
    backward(2)
    swap_partial(2)
    backward(3)
    swap_partial(3)
    bsib_copies[2].wait_recv()
    far_send[...] = (d_acc[2, core] + sib_recv[2].astype(F32)).astype(BF16)
    bfar = {}
    for way, col, start in ((0, right, 0), (1, left, half)):
        copy = remote(far_send.at[pl.ds(start, half)], far_recv.at[way], bfar_ssem.at[way], bfar_rsem.at[way], device(y, col, core))
        copy.start()
        pending.append(copy)
        bfar[way] = copy
    backward(1)
    swap_partial(1)
    bnear = {}
    for way, rel, col, start in ((1, 3, left, half), (0, 1, right, 0)):
        bsib_copies[rel].wait_recv()
        bfar[way].wait_recv()
        total = d_acc[rel, core] + sib_recv[rel].astype(F32)
        near_send[way] = total.astype(BF16)
        near_send[way, start:start + half] = (total[start:start + half] + far_recv[way].astype(F32)).astype(BF16)
        copy = remote(near_send.at[way], near_recv.at[way], bnear_ssem.at[way], bnear_rsem.at[way], device(y, col, core))
        copy.start()
        pending.append(copy)
        bnear[way] = copy
    backward(0)
    swap_partial(0)

    def finish_backward(yq, carry):
        o_stage[1, yq] = jnp.transpose(dq_acc[yq] * scale).astype(BF16)
        return carry

    lax.fori_loop(0, heads, finish_backward, 0)
    dq_copies = exchange(5, lambda ty, tc: o_stage.at[1, ty, lanes(tc, rows)], lambda ty, tc: dq_out.at[:, lanes(mine, width)])

    bsib_copies[0].wait_recv()
    bnear[0].wait_recv()
    bnear[1].wait_recv()
    factor = jnp.where(core == 0, scale, 1.0)
    o_stage[2] = ((d_acc[0, core] + sib_recv[0].astype(F32) + near_recv[0].astype(F32) + near_recv[1].astype(F32)) * factor).astype(BF16)
    dkv_copies = exchange(6, lambda ty, tc: o_stage.at[2, ty, lanes(tc, rows)], lambda ty, tc: dkv_out.at[:, lanes(core * heads + y, width)])

    for copies in (o_copies, ds_copies, dq_copies, dkv_copies):
        for key in offsets + [(0, 0)]:
            arrive(copies, key)
    for copy in pending:
        copy.wait_send()


def far_attention(q2, kv2, do2, sinks, kv_heads, num_shards):
    rows = q2.shape[0]
    num_heads = sinks.shape[0]
    width = q2.shape[1] // num_heads
    cores = num_heads // kv_heads
    cols = num_shards // num_heads
    assert cols == 4 and kv_heads == 4 and cores == 2
    pair = cores * rows
    full = (kv_heads, pair, width)
    vm, dma = pltpu.VMEM, pltpu.SemaphoreType.DMA
    scratch = [
        vm(full, BF16), vm(full, BF16), vm((2, cols) + full, BF16),
        vm((kv_heads, width, pair), F32), vm((kv_heads, width, pair), F32),
        vm((kv_heads, 1, pair), F32), vm((kv_heads, 1, pair), F32), vm((kv_heads, 1, pair), F32),
        vm((cols, 2) + full, F32), vm((3,) + full, BF16), vm((num_heads, 8, 128), F32),
        vm((cols,) + full, BF16), vm((cols,) + full, BF16), vm(full, BF16), vm((2, kv_heads // 2, pair, width), BF16),
        vm((2,) + full, BF16), vm((2,) + full, BF16),
        dma((7, kv_heads, cores)), dma((7, kv_heads, cores)), dma((cols, kv_heads)), dma((cols, kv_heads)),
        dma((2, kv_heads)), dma((2, kv_heads)), dma((kv_heads,)), dma((kv_heads,)),
        dma((cols,)), dma((cols,)), dma((2,)), dma((2,)), dma((2,)), dma((2,)),
    ]
    space = pl.BlockSpec(memory_space=pltpu.VMEM)
    return pl.pallas_call(
        functools.partial(far_attention_kernel, (kv_heads, cores, cols, rows, width)),
        out_shape=[jax.ShapeDtypeStruct((rows, num_heads * width), BF16), jax.ShapeDtypeStruct((rows, num_heads * width), BF16),
                   jax.ShapeDtypeStruct((rows, 2 * kv_heads * width), BF16), jax.ShapeDtypeStruct((num_heads, 8, 128), F32)],
        in_specs=[pl.BlockSpec(memory_space=pltpu.SMEM), space, space, space],
        out_specs=[space] * 4,
        scratch_shapes=scratch,
        compiler_params=pltpu.CompilerParams(collective_id=0, has_side_effects=True, vmem_limit_bytes=67043328),
        name='far_attention',
    )(sinks, q2, kv2, do2)


def solution(mesh):
    num_shards = mesh.shape['cp']
    forward_pairs = [(source, source + 1) for source in range(num_shards - 1)]
    backward_pairs = [(source + 1, source) for source in range(num_shards - 1)]
    row_spec = P('dp', 'cp')
    device_spec = P(('dp', 'cp'))
    whole_spec = P()

    def local_step(hidden, grad_out, norm_gain, w_qkv, b_qkv, w_out, b_out, attn_sinks):
        seq_dev = hidden.shape[1]
        num_heads = attn_sinks.shape[1]
        head_dim = w_out.shape[1] // num_heads
        kv_heads = (w_qkv.shape[2] // head_dim - num_heads) // 2
        logit_scale = head_dim ** -0.5
        shard_start = lax.axis_index('cp') * seq_dev
        row_pos = shard_start + jnp.arange(seq_dev)
        cos_tab, sin_tab = rope_tables(row_pos, head_dim)

        hid_one = hidden.astype(jnp.float32)
        query_one, keys_one, values_one, rms_one = norm_project(hid_one, norm_gain[0], w_qkv[0], b_qkv[0], cos_tab, sin_tab, num_heads, kv_heads)
        tail_rows = jnp.concatenate([keys_one[:, seq_dev - WINDOW:], values_one[:, seq_dev - WINDOW:]], axis=2)
        prev_rows = lax.ppermute(tail_rows, 'cp', forward_pairs)
        near_keys = jnp.concatenate([prev_rows[:, :, :kv_heads], keys_one], axis=1)
        near_values = jnp.concatenate([prev_rows[:, :, kv_heads:], values_one], axis=1)
        near_pos = jnp.concatenate([shard_start - WINDOW + jnp.arange(WINDOW), row_pos])
        attn_one, prob_one, probbf_one, sink_one = attend_forward(query_one, near_keys, near_values, attn_sinks[0], row_pos, near_pos, True, logit_scale)
        middle = (hid_one + dense_out(attn_one, w_out[0], b_out[0])).astype(jnp.bfloat16)

        hid_two = middle.astype(jnp.float32)
        query_two, keys_two, values_two, rms_two = norm_project(hid_two, norm_gain[1], w_qkv[1], b_qkv[1], cos_tab, sin_tab, num_heads, kv_heads)
        d_out_two = grad_out.astype(jnp.float32)
        d_attn_two = jnp.einsum('bsd,qd->bsq', grad_out, w_out[1], preferred_element_type=jnp.float32).astype(jnp.bfloat16)
        flat_two = jnp.concatenate([keys_two.reshape(seq_dev, -1), values_two.reshape(seq_dev, -1)], axis=1)
        attn_two, dq_two, own_two, dsink_wide = far_attention(query_two.reshape(seq_dev, -1), flat_two, d_attn_two.reshape(seq_dev, -1), attn_sinks[1], kv_heads, num_shards)
        attn_two = attn_two.reshape(1, seq_dev, -1)
        dq_two = dq_two.reshape(query_two.shape)
        own_two = own_two.reshape(1, seq_dev, 2 * kv_heads, head_dim)
        dsink_two = dsink_wide[:, 0, 0]
        output = (hid_two + dense_out(attn_two, w_out[1], b_out[1])).astype(jnp.bfloat16)
        dhid_two, dgain_two, dbias_two = project_backward(dq_two, own_two[:, :, :kv_heads], own_two[:, :, kv_heads:], hid_two, rms_two, norm_gain[1], w_qkv[1], cos_tab, sin_tab)
        d_middle = (d_out_two + dhid_two).astype(jnp.bfloat16)

        d_mid_f = d_middle.astype(jnp.float32)
        d_attn_one = jnp.einsum('bsd,qd->bsq', d_middle, w_out[0], preferred_element_type=jnp.float32).astype(jnp.bfloat16).reshape(query_one.shape)
        dq_one, dk_near, dv_near, dsink_one = attend_backward(d_attn_one, query_one, near_keys, near_values, prob_one, probbf_one, sink_one, logit_scale)
        near_grad = jnp.concatenate([dk_near, dv_near], axis=2)
        prev_grad = lax.ppermute(near_grad[:, :WINDOW].astype(jnp.bfloat16), 'cp', backward_pairs)
        own_grad = near_grad[:, WINDOW:]
        cut_row = seq_dev - WINDOW
        own_one = jnp.concatenate([own_grad[:, :cut_row], own_grad[:, cut_row:] + prev_grad.astype(jnp.float32)], axis=1).astype(jnp.bfloat16)
        dhid_one, dgain_one, dbias_one = project_backward(dq_one, own_one[:, :, :kv_heads], own_one[:, :, kv_heads:], hid_one, rms_one, norm_gain[0], w_qkv[0], cos_tab, sin_tab)
        d_hidden = (d_mid_f + dhid_one).astype(jnp.bfloat16)

        d_gain = jnp.stack([dgain_one, dgain_two])[None]
        d_bias_qkv = jnp.stack([dbias_one, dbias_two])[None]
        d_bias_out = jnp.stack([jnp.sum(d_mid_f, axis=(0, 1)), jnp.sum(d_out_two, axis=(0, 1))])[None]
        d_sinks = jnp.stack([dsink_one, dsink_two])[None]
        return output, d_hidden, d_gain, d_bias_qkv, d_bias_out, d_sinks

    return jax.shard_map(local_step, mesh=mesh, in_specs=(row_spec, row_spec, whole_spec, whole_spec, whole_spec, whole_spec, whole_spec, whole_spec), out_specs=(row_spec, row_spec, device_spec, device_spec, device_spec, device_spec), check_vma=False)
```

```python
import functools

import jax
import jax.numpy as jnp
import math
from jax import lax
from jax.experimental import pallas as pl
from jax.experimental.pallas import tpu as pltpu
from jax.sharding import PartitionSpec as P

WINDOW = 128
EPSILON = 1e-5
ROPE_THETA = 150000.0
YARN_FACTOR = 32.0
YARN_CONTEXT = 4096.0
YARN_ALPHA = 1.0
YARN_BETA = 32.0


def rope_tables(positions, head_dim):
    half_dim = head_dim // 2
    freq_steps = jnp.arange(half_dim, dtype=jnp.float32)
    freq_base = ROPE_THETA ** (freq_steps * 2.0 / head_dim)
    concentration = 0.1 * math.log(YARN_FACTOR) + 1.0
    low_edge = half_dim * math.log(YARN_CONTEXT / (YARN_BETA * 2.0 * math.pi)) / math.log(ROPE_THETA)
    high_edge = half_dim * math.log(YARN_CONTEXT / (YARN_ALPHA * 2.0 * math.pi)) / math.log(ROPE_THETA)
    ramp_pos = jnp.clip((freq_steps - low_edge) / (high_edge - low_edge), 0.0, 1.0)
    inv_freq = (1.0 - ramp_pos) / freq_base + ramp_pos / (YARN_FACTOR * freq_base)
    angles = positions.astype(jnp.float32)[:, None] * inv_freq[None, :]
    return jnp.cos(angles) * concentration, jnp.sin(angles) * concentration


MESH = pl.DeviceIdType.MESH
F32 = jnp.float32
BF16 = jnp.bfloat16


def far_attention_kernel(dims, sink_ref, q_ref, kv_ref, do_ref, o_out, dq_out, dkv_out, dsink_out,
                         q_all, do_all, kv_all, o_acc, dq_acc, m_ref, l_ref, delta_ref,
                         d_acc, o_stage, ds_stage, sib_send, sib_recv, far_send, far_recv, near_send, near_recv,
                         y_ssem, y_rsem, sib_ssem, sib_rsem, near_ssem, near_rsem, relay_ssem, relay_rsem,
                         bsib_ssem, bsib_rsem, bfar_ssem, bfar_rsem, bnear_ssem, bnear_rsem):
    heads, cores, cols, rows, width = dims
    pair = cores * rows
    scale = width ** -0.5
    me = lax.axis_index('cp')
    core = lax.rem(me, cores)
    x = lax.rem(me // cores, cols)
    y = me // (cores * cols)
    sib = lax.rem(core + 1, cores)

    def device(yy, xx, cc):
        return (yy * cols + xx) * cores + cc

    right = lax.rem(x + 1, cols)
    left = lax.rem(x + cols - 1, cols)
    far = lax.rem(x + 2, cols)
    offsets = [(dy, dc) for dy in (1, 3, 2, 0) for dc in range(cores) if (dy, dc) != (0, 0)]

    barrier = pltpu.get_barrier_semaphore()
    partners = [device(lax.rem(y + dy, heads), x, lax.rem(core + dc, cores)) for dy, dc in offsets]
    partners += [device(y, right, core), device(y, left, core)]
    for other in partners:
        pl.semaphore_signal(barrier, inc=1, device_id={'cp': other}, device_id_type=MESH)
    pl.semaphore_wait(barrier, len(partners))

    def remote(src, dst, ssem, rsem, target):
        return pltpu.make_async_remote_copy(src_ref=src, dst_ref=dst, send_sem=ssem, recv_sem=rsem,
                                            device_id={'cp': target}, device_id_type=MESH)

    pending = []

    def exchange(kind, src_of, dst_of):
        copies = {}
        for dy, dc in offsets + [(0, 0)]:
            ty, tc = lax.rem(y + dy, heads), lax.rem(core + dc, cores)
            if (dy, dc) == (0, 0):
                copy = pltpu.make_async_copy(src_of(ty, tc), dst_of(ty, tc), y_rsem.at[kind, dy, dc])
            else:
                copy = remote(src_of(ty, tc), dst_of(ty, tc), y_ssem.at[kind, dy, dc], y_rsem.at[kind, dy, dc], device(ty, x, tc))
                pending.append(copy)
            copy.start()
            copies[dy, dc] = copy
        return copies

    def arrive(copies, key):
        if key == (0, 0):
            copies[key].wait()
        else:
            copies[key].wait_recv()

    def lanes(block, size):
        return pl.ds(pl.multiple_of(block * size, size), size)

    my_rows = lanes(core, rows)
    kv_copies = exchange(0, lambda ty, tc: kv_ref.at[:, lanes(tc * heads + ty, width)],
                         lambda ty, tc: kv_all.at[tc, x, y, my_rows])
    q_copies = exchange(1, lambda ty, tc: q_ref.at[:, lanes(ty * cores + tc, width)],
                        lambda ty, tc: q_all.at[y, my_rows])
    do_copies = exchange(2, lambda ty, tc: do_ref.at[:, lanes(ty * cores + tc, width)],
                         lambda ty, tc: do_all.at[y, my_rows])

    sink = sink_ref[y * cores + core]
    m_ref[...] = jnp.zeros_like(m_ref) + sink
    l_ref[...] = jnp.ones_like(l_ref)
    o_acc[...] = jnp.zeros_like(o_acc)
    dq_acc[...] = jnp.zeros_like(dq_acc)

    order = (0, 1, 3, 2)
    sib_copies = {}
    near_copies = {}
    relay_copies = {}

    def to_sibling(rel, col, dy, piece):
        copy = remote(kv_all.at[core, col, piece], kv_all.at[core, col, piece], sib_ssem.at[rel, dy], sib_rsem.at[rel, dy], device(y, x, sib))
        copy.start()
        pending.append(copy)
        sib_copies[rel, dy] = copy

    def piece_of(dy):
        return lax.rem(y + heads - dy, heads)

    for dy in order:
        for dc in range(cores):
            arrive(kv_copies, (dy, dc))
        piece = piece_of(dy)
        for way, col in ((0, right), (1, left)):
            copy = remote(kv_all.at[core, x, piece], kv_all.at[core, x, piece], near_ssem.at[way, dy], near_rsem.at[way, dy], device(y, col, core))
            copy.start()
            pending.append(copy)
            near_copies[way, dy] = copy
        to_sibling(0, x, dy, piece)

    def relay(dy):
        piece = piece_of(dy)
        near_copies[0, dy].wait_recv()
        if dy in (0, 1):
            copy = remote(kv_all.at[core, left, piece], kv_all.at[core, left, piece], relay_ssem.at[dy], relay_rsem.at[dy], device(y, right, core))
            copy.start()
            pending.append(copy)
            relay_copies[dy] = copy
        to_sibling(3, left, dy, piece)
        near_copies[1, dy].wait_recv()
        if dy in (2, 3):
            copy = remote(kv_all.at[core, right, piece], kv_all.at[core, right, piece], relay_ssem.at[dy], relay_rsem.at[dy], device(y, left, core))
            copy.start()
            pending.append(copy)
            relay_copies[dy] = copy
        to_sibling(1, right, dy, piece)

    def scores(key_blk, query_blk, masked):
        out = lax.dot_general(key_blk, query_blk, (((1,), (1,)), ((), ())), preferred_element_type=F32) * scale
        if masked:
            key_pos = lax.broadcasted_iota(jnp.int32, out.shape, 0)
            query_pos = lax.broadcasted_iota(jnp.int32, out.shape, 1)
            out = jnp.where(key_pos <= query_pos, out, -jnp.inf)
        return out

    def forward_block(col, yk, yq, masked):
        value_blk = kv_all[1, col, yk]
        logits = scores(kv_all[0, col, yk], q_all[yq], masked)
        old_peak = m_ref[yq]
        peak = jnp.maximum(old_peak, jnp.max(logits, axis=0, keepdims=True))
        shrink = jnp.exp(old_peak - peak)
        weight = jnp.exp(logits - peak)
        m_ref[yq] = peak
        l_ref[yq] = l_ref[yq] * shrink + jnp.sum(weight, axis=0, keepdims=True)
        o_acc[yq] = o_acc[yq] * shrink + lax.dot_general(value_blk, weight.astype(BF16), (((0,), (0,)), ((), ())), preferred_element_type=F32)

    def backward_block(rel, col, yk, yq, masked):
        key_blk, value_blk = kv_all[0, col, yk], kv_all[1, col, yk]
        query_blk, grad_blk = q_all[yq], do_all[yq]
        prob = jnp.exp(scores(key_blk, query_blk, masked) - m_ref[yq])
        d_prob = lax.dot_general(value_blk, grad_blk, (((1,), (1,)), ((), ())), preferred_element_type=F32).astype(BF16).astype(F32)
        d_score = (prob * (d_prob - delta_ref[yq])).astype(BF16)
        d_acc[rel, 1, yk] += jnp.dot(prob.astype(BF16), grad_blk, preferred_element_type=F32)
        d_acc[rel, 0, yk] += jnp.dot(d_score, query_blk, preferred_element_type=F32)
        dq_acc[yq] += lax.dot_general(key_blk, d_score, (((0,), (0,)), ((), ())), preferred_element_type=F32)

    def sweep(block, rel, col):
        skip = 1 if rel == 0 else jnp.where(col > x, 1, 0)

        def over_keys(yk, carry):
            if rel == 0:
                block(yk, yk, True)

            def over_queries(yq, inner):
                block(yk, yq, False)
                return inner

            lax.fori_loop(yk + skip, heads, over_queries, 0)
            return carry

        lax.fori_loop(0, heads, over_keys, 0)

    cols_of = {0: x, 1: right, 2: far, 3: left}

    def forward(rel):
        col = cols_of[rel]
        sweep(lambda yk, yq, masked: forward_block(col, yk, yq, masked), rel, col)

    def backward(rel):
        col = cols_of[rel]
        sweep(lambda yk, yq, masked: backward_block(rel, col, yk, yq, masked), rel, col)

    def await_sibling(rel):
        for dy in order:
            sib_copies[rel, dy].wait_recv()

    relay(0)
    relay(1)
    for key in offsets + [(0, 0)]:
        arrive(q_copies, key)
    await_sibling(0)
    forward(0)
    relay(3)
    relay(2)
    d_acc[...] = jnp.zeros_like(d_acc)
    await_sibling(1)
    await_sibling(3)
    forward(1)
    forward(3)
    for dy in order:
        relay_copies[dy].wait_recv()
        to_sibling(2, far, dy, piece_of(dy))
    await_sibling(2)
    forward(2)

    for key in offsets + [(0, 0)]:
        arrive(do_copies, key)

    def finish_forward(yq, carry):
        attn = o_acc[yq] / l_ref[yq]
        lse = m_ref[yq] + jnp.log(l_ref[yq])
        delta = jnp.sum(attn * jnp.transpose(do_all[yq].astype(F32)), axis=0, keepdims=True)
        o_stage[0, yq] = jnp.transpose(attn).astype(BF16)
        m_ref[yq] = lse
        delta_ref[yq] = delta
        contribution = -jnp.exp(sink - lse) * delta
        for part in range(cores):
            total = jnp.sum(contribution[:, part * rows:(part + 1) * rows], axis=1, keepdims=True)
            ds_stage[yq * cores + part] = jnp.zeros(ds_stage.shape[1:], F32) + total
        return carry

    lax.fori_loop(0, heads, finish_forward, 0)

    mine = y * cores + core
    o_copies = exchange(3, lambda ty, tc: o_stage.at[0, ty, lanes(tc, rows)], lambda ty, tc: o_out.at[:, lanes(mine, width)])
    ds_copies = exchange(4, lambda ty, tc: ds_stage.at[ty * cores + tc], lambda ty, tc: dsink_out.at[mine])

    bsib_copies = {}

    def swap_partial(rel):
        sib_send[rel] = d_acc[rel, sib].astype(BF16)
        copy = remote(sib_send.at[rel], sib_recv.at[rel], bsib_ssem.at[rel], bsib_rsem.at[rel], device(y, x, sib))
        copy.start()
        pending.append(copy)
        bsib_copies[rel] = copy

    half = heads // 2
    backward(2)
    swap_partial(2)
    backward(3)
    swap_partial(3)
    bsib_copies[2].wait_recv()
    far_send[...] = (d_acc[2, core] + sib_recv[2].astype(F32)).astype(BF16)
    bfar = {}
    for way, col, start in ((0, right, 0), (1, left, half)):
        copy = remote(far_send.at[pl.ds(start, half)], far_recv.at[way], bfar_ssem.at[way], bfar_rsem.at[way], device(y, col, core))
        copy.start()
        pending.append(copy)
        bfar[way] = copy
    backward(1)
    swap_partial(1)
    bnear = {}
    for way, rel, col, start in ((1, 3, left, half), (0, 1, right, 0)):
        bsib_copies[rel].wait_recv()
        bfar[way].wait_recv()
        total = d_acc[rel, core] + sib_recv[rel].astype(F32)
        near_send[way] = total.astype(BF16)
        near_send[way, start:start + half] = (total[start:start + half] + far_recv[way].astype(F32)).astype(BF16)
        copy = remote(near_send.at[way], near_recv.at[way], bnear_ssem.at[way], bnear_rsem.at[way], device(y, col, core))
        copy.start()
        pending.append(copy)
        bnear[way] = copy
    backward(0)
    swap_partial(0)

    def finish_backward(yq, carry):
        o_stage[1, yq] = jnp.transpose(dq_acc[yq] * scale).astype(BF16)
        return carry

    lax.fori_loop(0, heads, finish_backward, 0)
    dq_copies = exchange(5, lambda ty, tc: o_stage.at[1, ty, lanes(tc, rows)], lambda ty, tc: dq_out.at[:, lanes(mine, width)])

    bsib_copies[0].wait_recv()
    bnear[0].wait_recv()
    bnear[1].wait_recv()
    factor = jnp.where(core == 0, scale, 1.0)
    o_stage[2] = ((d_acc[0, core] + sib_recv[0].astype(F32) + near_recv[0].astype(F32) + near_recv[1].astype(F32)) * factor).astype(BF16)
    dkv_copies = exchange(6, lambda ty, tc: o_stage.at[2, ty, lanes(tc, rows)], lambda ty, tc: dkv_out.at[:, lanes(core * heads + y, width)])

    for copies in (o_copies, ds_copies, dq_copies, dkv_copies):
        for key in offsets + [(0, 0)]:
            arrive(copies, key)
    for copy in pending:
        copy.wait_send()


def far_attention(q2, kv2, do2, sinks, kv_heads, num_shards):
    rows = q2.shape[0]
    num_heads = sinks.shape[0]
    width = q2.shape[1] // num_heads
    cores = num_heads // kv_heads
    cols = num_shards // num_heads
    assert cols == 4 and kv_heads == 4 and cores == 2
    pair = cores * rows
    full = (kv_heads, pair, width)
    vm, dma = pltpu.VMEM, pltpu.SemaphoreType.DMA
    scratch = [
        vm(full, BF16), vm(full, BF16), vm((2, cols) + full, BF16),
        vm((kv_heads, width, pair), F32), vm((kv_heads, width, pair), F32),
        vm((kv_heads, 1, pair), F32), vm((kv_heads, 1, pair), F32), vm((kv_heads, 1, pair), F32),
        vm((cols, 2) + full, F32), vm((3,) + full, BF16), vm((num_heads, 8, 128), F32),
        vm((cols,) + full, BF16), vm((cols,) + full, BF16), vm(full, BF16), vm((2, kv_heads // 2, pair, width), BF16),
        vm((2,) + full, BF16), vm((2,) + full, BF16),
        dma((7, kv_heads, cores)), dma((7, kv_heads, cores)), dma((cols, kv_heads)), dma((cols, kv_heads)),
        dma((2, kv_heads)), dma((2, kv_heads)), dma((kv_heads,)), dma((kv_heads,)),
        dma((cols,)), dma((cols,)), dma((2,)), dma((2,)), dma((2,)), dma((2,)),
    ]
    space = pl.BlockSpec(memory_space=pltpu.VMEM)
    return pl.pallas_call(
        functools.partial(far_attention_kernel, (kv_heads, cores, cols, rows, width)),
        out_shape=[jax.ShapeDtypeStruct((rows, num_heads * width), BF16), jax.ShapeDtypeStruct((rows, num_heads * width), BF16),
                   jax.ShapeDtypeStruct((rows, 2 * kv_heads * width), BF16), jax.ShapeDtypeStruct((num_heads, 8, 128), F32)],
        in_specs=[pl.BlockSpec(memory_space=pltpu.SMEM), space, space, space],
        out_specs=[space] * 4,
        scratch_shapes=scratch,
        compiler_params=pltpu.CompilerParams(collective_id=0, has_side_effects=True, vmem_limit_bytes=67043328),
        name='far_attention',
    )(sinks, q2, kv2, do2)


def rotate_tile(tile, cos, sin, width):
    half = width // 2
    parts = []
    for start in range(0, tile.shape[1], width):
        first, second = tile[:, start:start + half], tile[:, start + half:start + width]
        parts += [first * cos - second * sin, second * cos + first * sin]
    return jnp.concatenate(parts, axis=1)


def near_mask(shape, me):
    key_row = lax.broadcasted_iota(jnp.int32, shape, 0)
    query_row = lax.broadcasted_iota(jnp.int32, shape, 1)
    first_key = jnp.where(me > 0, 0, WINDOW)
    return (key_row >= first_key) & (key_row - WINDOW <= query_row) & (key_row >= query_row)


def forward_kernel(dims, sink_ref, hid_ref, grad_ref, gain_ref, bqkv_ref, bout_ref, cos_ref, sin_ref, wqkv_hbm, wout_hbm,
                   q_one, ext_one, lse_one, mid_out, q_two, kv_two, do_two,
                   ring, wout_one, wout_two, normed, attn, ring_sem, wout_sem, halo_ssem, halo_rsem):
    kv_heads, num_heads, rows, width, model, num_shards, tile, depth = dims
    me = lax.axis_index('cp')
    follow, before = lax.rem(me + 1, num_shards), lax.rem(me + num_shards - 1, num_shards)
    group = num_heads // kv_heads
    qw = num_heads * width
    kw = kv_heads * width
    q_tiles, k_tiles = qw // tile, kw // tile
    per_layer = q_tiles + 2 * k_tiles
    scale = width ** -0.5

    def weight(seq):
        layer, spot = seq // per_layer, lax.rem(seq, per_layer)
        col = pl.multiple_of(lax.rem(spot + q_tiles, per_layer) * tile, tile)
        slot = lax.rem(seq, depth)
        return pltpu.make_async_copy(wqkv_hbm.at[layer, :, pl.ds(col, tile)], ring.at[slot], ring_sem.at[slot])

    for seq in range(depth):
        weight(seq).start()

    barrier = pltpu.get_barrier_semaphore()
    for other in (follow, before):
        pl.semaphore_signal(barrier, inc=1, device_id={'cp': other}, device_id_type=MESH)
    pl.semaphore_wait(barrier, 2)

    def normalize(source, layer):
        hid = source[...].astype(F32)
        inv = lax.rsqrt(jnp.mean(hid * hid, axis=-1, keepdims=True) + EPSILON)
        normed[...] = (hid * inv * gain_ref[layer:layer + 1, :]).astype(BF16)

    def project(layer, first, count, rotate, store):
        def step(i, carry):
            seq = layer * per_layer + first + i
            weight(seq).wait()
            col = pl.multiple_of((first + q_tiles + i) % per_layer * tile, tile)
            out = jnp.dot(normed[...], ring[lax.rem(seq, depth)], preferred_element_type=F32) + bqkv_ref[layer:layer + 1, pl.ds(col, tile)]
            if rotate:
                out = rotate_tile(out, cos_ref[...], sin_ref[...], width)
            store(i, out.astype(BF16))

            @pl.when(seq + depth < 2 * per_layer)
            def _():
                weight(seq + depth).start()
            return carry

        lax.fori_loop(0, count, step, 0)

    def at(col):
        return pl.ds(pl.multiple_of(col * tile, tile), tile)

    def halo(i):
        return pltpu.make_async_remote_copy(src_ref=ext_one.at[pl.ds(rows, WINDOW), at(i)], dst_ref=ext_one.at[pl.ds(0, WINDOW), at(i)],
                                            send_sem=halo_ssem.at[i], recv_sem=halo_rsem.at[i], device_id={'cp': follow}, device_id_type=MESH)

    def store_near(base):
        def store(i, out):
            ext_one[pl.ds(WINDOW, rows), at(base + i)] = out
            halo(base + i).start()
        return store

    def store_flat(ref, base):
        def store(i, out):
            ref[:, at(base + i)] = out
        return store

    normalize(hid_ref, 0)
    project(0, 0, k_tiles, True, store_near(0))
    project(0, k_tiles, k_tiles, False, store_near(k_tiles))
    load_two = pltpu.make_async_copy(wout_hbm.at[1], wout_two, wout_sem.at[1])
    load_two.start()
    project(0, 2 * k_tiles, q_tiles, True, store_flat(q_one, 0))
    load_one = pltpu.make_async_copy(wout_hbm.at[0], wout_one, wout_sem.at[0])
    load_one.start()

    load_two.wait()

    def attn_grad(i, carry):
        do_two[:, at(i)] = lax.dot_general(grad_ref[...], wout_two[at(i), :], (((1,), (1,)), ((), ())), preferred_element_type=F32).astype(BF16)
        return carry

    lax.fori_loop(0, q_tiles, attn_grad, 0)
    for i in range(2 * k_tiles):
        halo(i).wait_recv()

    def near_head(h, carry):
        kv = h // group
        key_cols = pl.ds(pl.multiple_of(kv * width, width), width)
        value_cols = pl.ds(pl.multiple_of(kw + kv * width, width), width)
        head_cols = pl.ds(pl.multiple_of(h * width, width), width)
        logits = lax.dot_general(ext_one[:, key_cols], q_one[:, head_cols], (((1,), (1,)), ((), ())), preferred_element_type=F32) * scale
        logits = jnp.where(near_mask(logits.shape, me), logits, -jnp.inf)
        sink = sink_ref[0, h]
        peak = jnp.maximum(jnp.max(logits, axis=0, keepdims=True), sink)
        weights = jnp.exp(logits - peak)
        total = jnp.sum(weights, axis=0, keepdims=True) + jnp.exp(sink - peak)
        prob = (weights / total).astype(BF16)
        lse_one[h] = peak + jnp.log(total)
        attn[:, head_cols] = lax.dot_general(prob, ext_one[:, value_cols], (((0,), (0,)), ((), ())), preferred_element_type=F32).astype(BF16)
        return carry

    lax.fori_loop(0, num_heads, near_head, 0)
    load_one.wait()

    def mix(i, carry):
        out = jnp.dot(attn[...], wout_one[:, at(i)], preferred_element_type=F32)
        mid_out[:, at(i)] = (hid_ref[:, at(i)].astype(F32) + (out + bout_ref[0:1, at(i)])).astype(BF16)
        return carry

    lax.fori_loop(0, model // tile, mix, 0)
    normalize(mid_out, 1)
    project(1, 0, k_tiles, True, store_flat(kv_two, 0))
    project(1, k_tiles, k_tiles, False, store_flat(kv_two, k_tiles))
    project(1, 2 * k_tiles, q_tiles, True, store_flat(q_two, 0))
    for i in range(2 * k_tiles):
        halo(i).wait_send()


def backward_kernel(dims, sink_ref, o_two, dq_two, dkv_two, hid_ref, mid_ref, grad_ref, q_one, ext_one, lse_one, gain_ref, bout_ref, cos_ref, sin_ref, wqkv_hbm, wout_hbm,
                    out_ref, d_hid_ref, d_gain_ref, d_bqkv_ref, d_bout_ref, d_sink_ref,
                    ring, wout_one, wout_two, d_proj, d_norm, d_mid, d_attn, d_own, halo_send, halo_recv, ring_sem, wout_sem, halo_ssem, halo_rsem):
    kv_heads, num_heads, rows, width, model, num_shards, tile, depth = dims
    me = lax.axis_index('cp')
    follow, before = lax.rem(me + 1, num_shards), lax.rem(me + num_shards - 1, num_shards)
    group = num_heads // kv_heads
    qw = num_heads * width
    kw = kv_heads * width
    tiles = model // tile
    scale = width ** -0.5

    def weight(seq):
        layer, spot = 1 - seq // tiles, lax.rem(seq, tiles)
        slot = lax.rem(seq, depth)
        return pltpu.make_async_copy(wqkv_hbm.at[layer, pl.ds(pl.multiple_of(spot * tile, tile), tile), :], ring.at[slot], ring_sem.at[slot])

    for seq in range(depth):
        weight(seq).start()
    load_one = pltpu.make_async_copy(wout_hbm.at[0], wout_one, wout_sem.at[0])
    load_two = pltpu.make_async_copy(wout_hbm.at[1], wout_two, wout_sem.at[1])

    barrier = pltpu.get_barrier_semaphore()
    for other in (follow, before):
        pl.semaphore_signal(barrier, inc=1, device_id={'cp': other}, device_id_type=MESH)
    pl.semaphore_wait(barrier, 2)

    def at(col):
        return pl.ds(pl.multiple_of(col * tile, tile), tile)

    def head_at(h):
        return pl.ds(pl.multiple_of(h * width, width), width)

    def unrotate(layer, h, grad):
        out = rotate_tile(grad.astype(F32), cos_ref[...], -sin_ref[...], width)
        put(layer, h, out)

    def put(layer, h, out):
        d_bqkv_ref[layer:layer + 1, head_at(h)] = jnp.sum(out, axis=0, keepdims=True)
        d_proj[:, head_at(h)] = out.astype(BF16)

    def project_back(layer, source, skip_ref, target):
        def step(i, carry):
            seq = (1 - layer) * tiles + i
            weight(seq).wait()
            out = lax.dot_general(d_proj[...], ring[lax.rem(seq, depth)], (((1,), (1,)), ((), ())), preferred_element_type=F32)
            d_norm[:, at(i)] = out.astype(BF16)

            @pl.when(seq + depth < 2 * tiles)
            def _():
                weight(seq + depth).start()
            return carry

        lax.fori_loop(0, tiles, step, 0)
        hid = source[...].astype(F32)
        inv = lax.rsqrt(jnp.mean(hid * hid, axis=-1, keepdims=True) + EPSILON)
        grad = d_norm[...].astype(F32)
        d_gain_ref[layer:layer + 1, :] = jnp.sum(grad * hid * inv, axis=0, keepdims=True)
        unit = grad * gain_ref[layer:layer + 1, :]
        d_hid = inv * unit - hid * (inv * inv * inv) * jnp.mean(unit * hid, axis=-1, keepdims=True)
        skip = skip_ref[...].astype(F32)
        target[...] = (skip + d_hid).astype(BF16)

    def two_heads(h, carry):
        unrotate(1, h, dq_two[:, head_at(h)])
        return carry

    def two_keys(h, carry):
        unrotate(1, num_heads + h, dkv_two[:, head_at(h)])
        return carry

    def two_values(h, carry):
        put(1, num_heads + kv_heads + h, dkv_two[:, head_at(kv_heads + h)].astype(F32))
        return carry

    lax.fori_loop(0, num_heads, two_heads, 0)
    lax.fori_loop(0, kv_heads, two_keys, 0)
    lax.fori_loop(0, kv_heads, two_values, 0)
    load_one.start()
    project_back(1, mid_ref, grad_ref, d_mid)
    load_two.start()
    d_bout_ref[1:2, :] = jnp.sum(grad_ref[...].astype(F32), axis=0, keepdims=True)
    d_bout_ref[0:1, :] = jnp.sum(d_mid[...].astype(F32), axis=0, keepdims=True)
    load_one.wait()

    def attn_grad(i, carry):
        d_attn[:, at(i)] = lax.dot_general(d_mid[...], wout_one[at(i), :], (((1,), (1,)), ((), ())), preferred_element_type=F32).astype(BF16)
        return carry

    lax.fori_loop(0, qw // tile, attn_grad, 0)

    def halo(g):
        return pltpu.make_async_remote_copy(src_ref=halo_send.at[g], dst_ref=halo_recv.at[g], send_sem=halo_ssem.at[g], recv_sem=halo_rsem.at[g],
                                            device_id={'cp': before}, device_id_type=MESH)

    def near_group(g, carry):
        key_blk, value_blk = ext_one[:, head_at(g)], ext_one[:, head_at(kv_heads + g)]
        d_key = d_value = None
        for part in range(group):
            h = g * group + part
            query_blk, grad_blk = q_one[:, head_at(h)], d_attn[:, head_at(h)]
            logits = lax.dot_general(key_blk, query_blk, (((1,), (1,)), ((), ())), preferred_element_type=F32) * scale
            logits = jnp.where(near_mask(logits.shape, me), logits, -jnp.inf)
            lse = lse_one[h]
            prob = jnp.exp(logits - lse)
            d_prob = lax.dot_general(value_blk, grad_blk, (((1,), (1,)), ((), ())), preferred_element_type=F32).astype(BF16).astype(F32)
            delta = jnp.sum(prob * d_prob, axis=0, keepdims=True)
            d_score = (prob * (d_prob - delta)).astype(BF16)
            d_query = lax.dot_general(d_score, key_blk, (((0,), (0,)), ((), ())), preferred_element_type=F32) * scale
            unrotate(0, h, d_query.astype(BF16))
            d_sink = -jnp.sum(jnp.exp(sink_ref[0, h] - lse) * delta, axis=1, keepdims=True)
            d_sink_ref[h] = jnp.zeros(d_sink_ref.shape[1:], F32) + d_sink
            one_key = jnp.dot(d_score, query_blk, preferred_element_type=F32)
            one_value = jnp.dot(prob.astype(BF16), grad_blk, preferred_element_type=F32)
            d_key = one_key if d_key is None else d_key + one_key
            d_value = one_value if d_value is None else d_value + one_value
        d_key = d_key * scale
        halo_send[g, 0] = d_key[:WINDOW].astype(BF16)
        halo_send[g, 1] = d_value[:WINDOW].astype(BF16)
        d_own[0, g] = d_key[WINDOW:]
        d_own[1, g] = d_value[WINDOW:]
        halo(g).start()
        return carry

    lax.fori_loop(0, kv_heads, near_group, 0)
    load_two.wait()

    def mix(i, carry):
        out = jnp.dot(o_two[...], wout_two[:, at(i)], preferred_element_type=F32)
        out_ref[:, at(i)] = (mid_ref[:, at(i)].astype(F32) + (out + bout_ref[1:2, at(i)])).astype(BF16)
        return carry

    lax.fori_loop(0, tiles, mix, 0)
    for g in range(kv_heads):
        halo(g).wait_recv()
    tail = pl.ds(rows - WINDOW, WINDOW)

    def near_finish(g, carry):
        for kind in range(2):
            d_own[kind, g, tail] += halo_recv[g, kind].astype(F32)
        unrotate(0, num_heads + g, d_own[0, g].astype(BF16))
        put(0, num_heads + kv_heads + g, d_own[1, g].astype(BF16).astype(F32))
        return carry

    lax.fori_loop(0, kv_heads, near_finish, 0)
    project_back(0, hid_ref, d_mid, d_hid_ref)
    for g in range(kv_heads):
        halo(g).wait_send()


def forward_call(hid, grad, gain, bqkv, bout, cos, sin, wqkv, wout, sinks, kv_heads, num_shards):
    rows, model = hid.shape
    num_heads = sinks.shape[1]
    width = wout.shape[1] // num_heads
    qw, kw = num_heads * width, kv_heads * width
    tile, depth = 512, 4
    vm, dma = pltpu.VMEM, pltpu.SemaphoreType.DMA
    space, far = pl.BlockSpec(memory_space=pltpu.VMEM), pl.BlockSpec(memory_space=pl.ANY)
    shape = jax.ShapeDtypeStruct
    return pl.pallas_call(
        functools.partial(forward_kernel, (kv_heads, num_heads, rows, width, model, num_shards, tile, depth)),
        out_shape=[shape((rows, qw), BF16), shape((WINDOW + rows, 2 * kw), BF16), shape((num_heads, 1, rows), F32), shape((rows, model), BF16),
                   shape((rows, qw), BF16), shape((rows, 2 * kw), BF16), shape((rows, qw), BF16)],
        in_specs=[pl.BlockSpec(memory_space=pltpu.SMEM)] + [space] * 7 + [far] * 2,
        out_specs=[space] * 7,
        scratch_shapes=[vm((depth, model, tile), BF16), vm((qw, model), BF16), vm((qw, model), BF16), vm((rows, model), BF16), vm((rows, qw), BF16),
                        dma((depth,)), dma((2,)), dma((2 * kw // tile,)), dma((2 * kw // tile,))],
        compiler_params=pltpu.CompilerParams(collective_id=1, has_side_effects=True, vmem_limit_bytes=67043328),
        name='forward_dense',
    )(sinks, hid, grad, gain, bqkv, bout, cos, sin, wqkv, wout)


def backward_call(o_two, dq_two, dkv_two, hid, mid, grad, q_one, ext_one, lse_one, gain, bout, cos, sin, wqkv, wout, sinks, kv_heads, num_shards):
    rows, model = hid.shape
    num_heads = sinks.shape[1]
    width = wout.shape[1] // num_heads
    qw, kw = num_heads * width, kv_heads * width
    tile, depth = 512, 3
    vm, dma = pltpu.VMEM, pltpu.SemaphoreType.DMA
    space, far = pl.BlockSpec(memory_space=pltpu.VMEM), pl.BlockSpec(memory_space=pl.ANY)
    shape = jax.ShapeDtypeStruct
    return pl.pallas_call(
        functools.partial(backward_kernel, (kv_heads, num_heads, rows, width, model, num_shards, tile, depth)),
        out_shape=[shape((rows, model), BF16), shape((rows, model), BF16), shape((2, model), F32), shape((2, qw + 2 * kw), F32), shape((2, model), F32),
                   shape((num_heads, 8, 128), F32)],
        in_specs=[pl.BlockSpec(memory_space=pltpu.SMEM)] + [space] * 13 + [far] * 2,
        out_specs=[space] * 6,
        scratch_shapes=[vm((depth, tile, qw + 2 * kw), BF16), vm((qw, model), BF16), vm((qw, model), BF16), vm((rows, qw + 2 * kw), BF16), vm((rows, model), BF16),
                        vm((rows, model), BF16), vm((rows, qw), BF16), vm((2, kv_heads, rows, width), F32),
                        vm((kv_heads, 2, WINDOW, width), BF16), vm((kv_heads, 2, WINDOW, width), BF16),
                        dma((depth,)), dma((2,)), dma((kv_heads,)), dma((kv_heads,))],
        compiler_params=pltpu.CompilerParams(collective_id=2, has_side_effects=True, vmem_limit_bytes=67043328),
        name='backward_dense',
    )(sinks, o_two, dq_two, dkv_two, hid, mid, grad, q_one, ext_one, lse_one, gain, bout, cos, sin, wqkv, wout)


def solution(mesh):
    num_shards = mesh.shape['cp']
    row_spec = P('dp', 'cp')
    device_spec = P(('dp', 'cp'))
    whole_spec = P()

    def local_step(hidden, grad_out, norm_gain, w_qkv, b_qkv, w_out, b_out, attn_sinks):
        seq_dev = hidden.shape[1]
        num_heads = attn_sinks.shape[1]
        head_dim = w_out.shape[1] // num_heads
        kv_heads = (w_qkv.shape[2] // head_dim - num_heads) // 2
        row_pos = lax.axis_index('cp') * seq_dev + jnp.arange(seq_dev)
        cos_tab, sin_tab = rope_tables(row_pos, head_dim)
        hid, grad = hidden[0], grad_out[0]

        query_one, near_one, lse_one, middle, query_two, flat_two, d_attn_two = forward_call(
            hid, grad, norm_gain, b_qkv, b_out, cos_tab, sin_tab, w_qkv, w_out, attn_sinks, kv_heads, num_shards)
        attn_two, dq_two, dkv_two, dsink_two = far_attention(query_two, flat_two, d_attn_two, attn_sinks[1], kv_heads, num_shards)
        output, d_hidden, d_gain, d_bias_qkv, d_bias_out, dsink_one = backward_call(
            attn_two, dq_two, dkv_two, hid, middle, grad, query_one, near_one, lse_one, norm_gain, b_out, cos_tab, sin_tab, w_qkv, w_out, attn_sinks, kv_heads, num_shards)
        d_sinks = jnp.stack([dsink_one[:, 0, 0], dsink_two[:, 0, 0]])
        return output[None], d_hidden[None], d_gain[None], d_bias_qkv[None], d_bias_out[None], d_sinks[None]

    return jax.shard_map(local_step, mesh=mesh, in_specs=(row_spec, row_spec, whole_spec, whole_spec, whole_spec, whole_spec, whole_spec, whole_spec), out_specs=(row_spec, row_spec, device_spec, device_spec, device_spec, device_spec), check_vma=False)
```

```python
import functools

import jax
import jax.numpy as jnp
import math
from jax import lax
from jax.experimental import pallas as pl
from jax.experimental.pallas import tpu as pltpu
from jax.sharding import PartitionSpec as P

WINDOW = 128
EPSILON = 1e-5
ROPE_THETA = 150000.0
YARN_FACTOR = 32.0
YARN_CONTEXT = 4096.0
YARN_ALPHA = 1.0
YARN_BETA = 32.0


def rope_tables(positions, head_dim):
    half_dim = head_dim // 2
    freq_steps = jnp.arange(half_dim, dtype=jnp.float32)
    freq_base = ROPE_THETA ** (freq_steps * 2.0 / head_dim)
    concentration = 0.1 * math.log(YARN_FACTOR) + 1.0
    low_edge = half_dim * math.log(YARN_CONTEXT / (YARN_BETA * 2.0 * math.pi)) / math.log(ROPE_THETA)
    high_edge = half_dim * math.log(YARN_CONTEXT / (YARN_ALPHA * 2.0 * math.pi)) / math.log(ROPE_THETA)
    ramp_pos = jnp.clip((freq_steps - low_edge) / (high_edge - low_edge), 0.0, 1.0)
    inv_freq = (1.0 - ramp_pos) / freq_base + ramp_pos / (YARN_FACTOR * freq_base)
    angles = positions.astype(jnp.float32)[:, None] * inv_freq[None, :]
    return jnp.cos(angles) * concentration, jnp.sin(angles) * concentration


MESH = pl.DeviceIdType.MESH
F32 = jnp.float32
BF16 = jnp.bfloat16


def far_attention_kernel(dims, sink_ref, q_ref, kv_ref, do_ref, o_out, dq_out, dkv_out, dsink_out,
                         q_all, do_all, kv_all, o_acc, dq_acc, m_ref, l_ref, delta_ref,
                         d_acc, o_stage, ds_stage, sib_send, sib_recv, far_send, far_recv, near_send, near_recv,
                         y_ssem, y_rsem, sib_ssem, sib_rsem, near_ssem, near_rsem, relay_ssem, relay_rsem,
                         bsib_ssem, bsib_rsem, bfar_ssem, bfar_rsem, bnear_ssem, bnear_rsem):
    heads, cores, cols, rows, width = dims
    pair = cores * rows
    scale = width ** -0.5
    me = lax.axis_index('cp')
    core = lax.rem(me, cores)
    x = lax.rem(me // cores, cols)
    y = me // (cores * cols)
    sib = lax.rem(core + 1, cores)

    def device(yy, xx, cc):
        return (yy * cols + xx) * cores + cc

    right = lax.rem(x + 1, cols)
    left = lax.rem(x + cols - 1, cols)
    far = lax.rem(x + 2, cols)
    offsets = [(dy, dc) for dy in (1, 3, 2, 0) for dc in range(cores) if (dy, dc) != (0, 0)]

    barrier = pltpu.get_barrier_semaphore()
    partners = [device(lax.rem(y + dy, heads), x, lax.rem(core + dc, cores)) for dy, dc in offsets]
    partners += [device(y, right, core), device(y, left, core)]
    for other in partners:
        pl.semaphore_signal(barrier, inc=1, device_id={'cp': other}, device_id_type=MESH)
    pl.semaphore_wait(barrier, len(partners))

    def remote(src, dst, ssem, rsem, target):
        return pltpu.make_async_remote_copy(src_ref=src, dst_ref=dst, send_sem=ssem, recv_sem=rsem,
                                            device_id={'cp': target}, device_id_type=MESH)

    pending = []

    def exchange(kind, src_of, dst_of):
        copies = {}
        for dy, dc in offsets + [(0, 0)]:
            ty, tc = lax.rem(y + dy, heads), lax.rem(core + dc, cores)
            if (dy, dc) == (0, 0):
                copy = pltpu.make_async_copy(src_of(ty, tc), dst_of(ty, tc), y_rsem.at[kind, dy, dc])
            else:
                copy = remote(src_of(ty, tc), dst_of(ty, tc), y_ssem.at[kind, dy, dc], y_rsem.at[kind, dy, dc], device(ty, x, tc))
                pending.append(copy)
            copy.start()
            copies[dy, dc] = copy
        return copies

    def arrive(copies, key):
        if key == (0, 0):
            copies[key].wait()
        else:
            copies[key].wait_recv()

    def lanes(block, size):
        return pl.ds(pl.multiple_of(block * size, size), size)

    my_rows = lanes(core, rows)
    kv_copies = exchange(0, lambda ty, tc: kv_ref.at[:, lanes(tc * heads + ty, width)],
                         lambda ty, tc: kv_all.at[tc, x, y, my_rows])
    q_copies = exchange(1, lambda ty, tc: q_ref.at[:, lanes(ty * cores + tc, width)],
                        lambda ty, tc: q_all.at[y, my_rows])
    do_copies = exchange(2, lambda ty, tc: do_ref.at[:, lanes(ty * cores + tc, width)],
                         lambda ty, tc: do_all.at[y, my_rows])

    sink = jnp.minimum(jnp.maximum(sink_ref[1, y * cores + core] * math.log2(math.e), -3.0e38), 3.0e38)
    m_ref[...] = jnp.zeros_like(m_ref) + sink
    l_ref[...] = jnp.ones_like(l_ref)
    o_acc[...] = jnp.zeros_like(o_acc)
    dq_acc[...] = jnp.zeros_like(dq_acc)

    order = (0, 1, 3, 2)
    sib_copies = {}
    near_copies = {}
    relay_copies = {}

    def to_sibling(rel, col, dy, piece):
        copy = remote(kv_all.at[core, col, piece], kv_all.at[core, col, piece], sib_ssem.at[rel, dy], sib_rsem.at[rel, dy], device(y, x, sib))
        copy.start()
        pending.append(copy)
        sib_copies[rel, dy] = copy

    def piece_of(dy):
        return lax.rem(y + heads - dy, heads)

    for dy in order:
        for dc in range(cores):
            arrive(kv_copies, (dy, dc))
        piece = piece_of(dy)
        for way, col in ((0, right), (1, left)):
            copy = remote(kv_all.at[core, x, piece], kv_all.at[core, x, piece], near_ssem.at[way, dy], near_rsem.at[way, dy], device(y, col, core))
            copy.start()
            pending.append(copy)
            near_copies[way, dy] = copy
        to_sibling(0, x, dy, piece)

    def relay(dy):
        piece = piece_of(dy)
        near_copies[0, dy].wait_recv()
        if dy in (0, 1):
            copy = remote(kv_all.at[core, left, piece], kv_all.at[core, left, piece], relay_ssem.at[dy], relay_rsem.at[dy], device(y, right, core))
            copy.start()
            pending.append(copy)
            relay_copies[dy] = copy
        to_sibling(3, left, dy, piece)
        near_copies[1, dy].wait_recv()
        if dy in (2, 3):
            copy = remote(kv_all.at[core, right, piece], kv_all.at[core, right, piece], relay_ssem.at[dy], relay_rsem.at[dy], device(y, left, core))
            copy.start()
            pending.append(copy)
            relay_copies[dy] = copy
        to_sibling(1, right, dy, piece)

    factor = scale * math.log2(math.e)

    def masked_scores(raw, start):
        key_pos = lax.broadcasted_iota(jnp.int32, raw.shape, 0)
        query_pos = lax.broadcasted_iota(jnp.int32, raw.shape, 1) + start
        return jnp.where(key_pos <= query_pos, raw, -jnp.inf)

    def raw_scores(key_blk, yq, masked):
        out = []
        for part in range(cores):
            raw = lax.dot_general(key_blk, q_all[yq, part * rows:(part + 1) * rows], (((1,), (1,)), ((), ())), preferred_element_type=F32)
            out.append(masked_scores(raw, part * rows) if masked else raw)
        return out

    def forward_block(col, yk, queries, masked):
        key_blk, value_blk = kv_all[0, col, yk], kv_all[1, col, yk]
        chains = [(yq, slice(part * rows, (part + 1) * rows)) for yq in queries for part in range(cores)]
        states = [(m_ref[yq, :, span], l_ref[yq, :, span], o_acc[yq, :, span]) for yq, span in chains]
        raws = [raw for yq in queries for raw in raw_scores(key_blk, yq, masked)]
        new = []
        for raw, (old, total, mixed) in zip(raws, states):
            peak = jnp.maximum(old, jnp.max(raw, axis=0, keepdims=True) * factor)
            shrink = jnp.exp2(old - peak)
            weight = jnp.exp2(raw * factor - peak)
            total = total * shrink + jnp.sum(weight, axis=0, keepdims=True)
            mixed = mixed * shrink + lax.dot_general(value_blk, weight.astype(BF16), (((0,), (0,)), ((), ())), preferred_element_type=F32)
            new.append((peak, total, mixed))
        for (yq, span), values in zip(chains, new):
            m_ref[yq, :, span], l_ref[yq, :, span], o_acc[yq, :, span] = values

    def forward_span(col, yk, low):
        count = heads - low
        loop(0, count // 2, lambda n: forward_block(col, yk, (low + 2 * n, low + 2 * n + 1), False))

        @pl.when(lax.rem(count, 2) == 1)
        def _():
            forward_block(col, yk, (heads - 1,), False)

    def backward_block(rel, col, yk, yq, masked):
        key_blk, value_blk = kv_all[0, col, yk], kv_all[1, col, yk]
        lse, delta = m_ref[yq], delta_ref[yq]
        raws = raw_scores(key_blk, yq, masked)
        probs, d_scores = [], []
        for part in range(cores):
            span = slice(part * rows, (part + 1) * rows)
            d_prob = lax.dot_general(value_blk, do_all[yq, span], (((1,), (1,)), ((), ())), preferred_element_type=F32).astype(BF16).astype(F32)
            prob = jnp.exp2(raws[part] * factor - lse[:, span])
            probs.append(prob.astype(BF16))
            d_scores.append((prob * (d_prob - delta[:, span])).astype(BF16))
        prob, d_score = jnp.concatenate(probs, axis=1), jnp.concatenate(d_scores, axis=1)
        d_value = d_acc[rel, 1, yk] + jnp.dot(prob, do_all[yq], preferred_element_type=F32)
        d_key = d_acc[rel, 0, yk] + jnp.dot(d_score, q_all[yq], preferred_element_type=F32)
        d_query = dq_acc[yq] + lax.dot_general(key_blk, d_score, (((0,), (0,)), ((), ())), preferred_element_type=F32)
        d_acc[rel, 1, yk] = d_value
        d_acc[rel, 0, yk] = d_key
        dq_acc[yq] = d_query

    def column(rel):
        return lax.rem(x + rel, cols)

    def loop(low, high, body):
        def step(i, carry):
            body(i)
            return carry
        lax.fori_loop(low, high, step, 0)

    def piece_sweep(block, rel, yk):
        col = column(rel)
        skip = (rel + x) // cols
        loop(yk + 1 - skip, heads, lambda yq: block(col, yk, yq))

    def forward_piece(rel, dy):
        col, piece = column(rel), piece_of(dy)
        remote(kv_all.at[core, col, piece], kv_all.at[core, col, piece], sib_ssem.at[rel, dy], sib_rsem.at[rel, dy], device(y, x, sib)).wait_recv()
        later = 1 - (rel + x) // cols
        forward_span(col, piece, piece + later)

    relay(0)
    relay(1)
    d_acc[...] = jnp.zeros_like(d_acc)
    for key in offsets + [(0, 0)]:
        arrive(q_copies, key)
    for dy in order:
        sib_copies[0, dy].wait_recv()

    def own_forward(yk):
        forward_block(x, yk, (yk,), True)
        forward_span(x, yk, yk + 1)

    loop(0, heads, own_forward)
    relay(3)
    loop(0, 4, lambda j: forward_piece(1 + 2 * lax.rem(j, 2), j // 2))
    relay(2)
    loop(0, 2, lambda j: forward_piece(1 + 2 * j, 3))
    for dy in (0, 1):
        relay_copies[dy].wait_recv()
        to_sibling(2, far, dy, piece_of(dy))
    loop(0, 2, lambda j: forward_piece(1 + 2 * j, 2))
    for dy in (3, 2):
        relay_copies[dy].wait_recv()
        to_sibling(2, far, dy, piece_of(dy))
    loop(0, heads, lambda j: forward_piece(2, j))

    for key in offsets + [(0, 0)]:
        arrive(do_copies, key)

    def finish_forward(yq):
        attn = o_acc[yq] / l_ref[yq]
        lse = m_ref[yq] + jnp.log2(l_ref[yq])
        delta = jnp.sum(attn * jnp.transpose(do_all[yq].astype(F32)), axis=0, keepdims=True)
        o_stage[0, yq] = jnp.transpose(attn).astype(BF16)
        m_ref[yq] = lse
        delta_ref[yq] = delta
        contribution = -jnp.exp2(sink - lse) * delta
        for part in range(cores):
            total = jnp.sum(contribution[:, part * rows:(part + 1) * rows], axis=1, keepdims=True)
            ds_stage[yq * cores + part] = jnp.zeros(ds_stage.shape[1:], F32) + total

    loop(0, heads, finish_forward)

    mine = y * cores + core
    o_copies = exchange(3, lambda ty, tc: o_stage.at[0, ty, lanes(tc, rows)], lambda ty, tc: o_out.at[:, lanes(mine, width)])
    ds_copies = exchange(4, lambda ty, tc: ds_stage.at[ty * cores + tc], lambda ty, tc: dsink_out.at[mine])

    def swap(rel, yk):
        return remote(sib_send.at[rel, yk], sib_recv.at[rel, yk], bsib_ssem.at[rel, yk], bsib_rsem.at[rel, yk], device(y, x, sib))

    def start_swap(rel, yk):
        sib_send[rel, yk] = d_acc[rel, sib, yk].astype(BF16)
        swap(rel, yk).start()

    def chip_total(rel, yk):
        swap(rel, yk).wait_recv()
        return d_acc[rel, core, yk] + sib_recv[rel, yk].astype(F32)

    def backward_piece(rel, yk):
        piece_sweep(lambda col, key, yq: backward_block(rel, col, key, yq, False), rel, yk)

    def far_copy(yk, way):
        target = lax.rem(x + 1 + 2 * way, cols)
        return remote(far_send.at[yk], far_recv.at[yk], bfar_ssem.at[yk], bfar_rsem.at[yk], device(y, target, core))

    def send_far(yk):
        far_send[yk] = chip_total(2, yk).astype(BF16)
        far_copy(yk, lax.rem(yk, 2)).start()

    def far_step(i):
        yk = heads - 1 - i
        backward_piece(2, yk)
        start_swap(2, yk)

        @pl.when(i > 0)
        def _():
            send_far(yk + 1)

    loop(0, heads, far_step)

    def near_key(t):
        side, turn = lax.rem(t, 2), t // 2
        from_left = 2 * lax.rem(turn, 2) + turn // 2
        return 3 - 2 * side, from_left + side * (heads - 1 - 2 * from_left)

    def near_copy(rel, yk):
        return remote(near_send.at[rel // 2, yk], near_recv.at[rel // 2, yk], bnear_ssem.at[rel // 2, yk], bnear_rsem.at[rel // 2, yk], device(y, column(rel), core))

    def send_near(t):
        rel, yk = near_key(t)
        total = chip_total(rel, yk)

        @pl.when(t < heads)
        def _():
            near_send[rel // 2, yk] = total.astype(BF16)

        @pl.when(t >= heads)
        def _():
            far_copy(yk, 0).wait_recv()
            near_send[rel // 2, yk] = (total + far_recv[yk].astype(F32)).astype(BF16)

        near_copy(rel, yk).start()

    def near_step(t):
        rel, yk = near_key(t)
        backward_piece(rel, yk)
        start_swap(rel, yk)

        @pl.when(t == 0)
        def _():
            send_far(0)

        @pl.when(t > 0)
        def _():
            send_near(t - 1)

    loop(0, 2 * heads, near_step)

    def scatter_copy(kind, src, dst, ty, dc):
        tc = lax.rem(core + dc, cores)
        return remote(src.at[ty, lanes(tc, rows)], dst, y_ssem.at[kind, ty, dc], y_rsem.at[kind, y, dc], device(ty, x, tc))

    def scatter(kind, src, dst, ty, act):
        for dc in range(1, cores):
            act(scatter_copy(kind, src, dst, ty, dc))

        @pl.when(ty != y)
        def _():
            act(scatter_copy(kind, src, dst, ty, 0))

    def scatter_wait(kind, src, dst):
        for source in range(heads):
            for dc in range(cores):
                copy = remote(src.at[source, lanes(core, rows)], dst, y_ssem.at[kind, source, dc], y_rsem.at[kind, source, dc], device(y, x, sib))
                if dc == 0:
                    @pl.when(source != y)
                    def _(copy=copy):
                        copy.wait_recv()
                else:
                    copy.wait_recv()
            scatter(kind, src, dst, source, lambda copy: copy.wait_send())

    dq_stage, dkv_stage = o_stage.at[1], o_stage.at[2]
    dq_dst = dq_out.at[:, lanes(mine, width)]
    dkv_dst = dkv_out.at[:, lanes(core * heads + y, width)]

    def own_backward(i):
        yq = heads - 1 - i
        loop(0, yq, lambda yk: backward_block(0, x, yk, yq, False))
        backward_block(0, x, yq, yq, True)
        start_swap(0, yq)

        @pl.when(i == 0)
        def _():
            send_near(2 * heads - 1)
        dq_stage[yq] = jnp.transpose(dq_acc[yq] * scale).astype(BF16)
        scatter(5, dq_stage, dq_dst, yq, lambda copy: copy.start())

    loop(0, heads, own_backward)
    dq_out[:, lanes(mine, width)] = dq_stage[y, lanes(core, rows)]
    key_scale = jnp.where(core == 0, scale, 1.0)

    def own_finish(i):
        yk = lax.rem(i + 1, heads)
        total = chip_total(0, yk)
        for rel in (1, 3):
            near_copy(rel, yk).wait_recv()
            total = total + near_recv[rel // 2, yk].astype(F32)
        dkv_stage[yk] = (total * key_scale).astype(BF16)
        scatter(6, dkv_stage, dkv_dst, yk, lambda copy: copy.start())

    loop(0, heads, own_finish)
    dkv_out[:, lanes(core * heads + y, width)] = dkv_stage[y, lanes(core, rows)]

    for copies in (o_copies, ds_copies):
        for key in offsets + [(0, 0)]:
            arrive(copies, key)
    scatter_wait(5, dq_stage, dq_dst)
    scatter_wait(6, dkv_stage, dkv_dst)

    def drain(yk):
        for rel in range(cols):
            swap(rel, yk).wait_send()
        far_copy(yk, 0).wait_send()
        for rel in (1, 3):
            near_copy(rel, yk).wait_send()

    loop(0, heads, drain)
    for copy in pending:
        copy.wait_send()


def far_attention(q2, kv2, do2, sinks, kv_heads, num_shards):
    rows = q2.shape[0]
    num_heads = sinks.shape[1]
    width = q2.shape[1] // num_heads
    cores = num_heads // kv_heads
    cols = num_shards // num_heads
    assert cols == 4 and kv_heads == 4 and cores == 2
    pair = cores * rows
    full = (kv_heads, pair, width)
    vm, dma = pltpu.VMEM, pltpu.SemaphoreType.DMA
    scratch = [
        vm(full, BF16), vm(full, BF16), vm((2, cols) + full, BF16),
        vm((kv_heads, width, pair), F32), vm((kv_heads, width, pair), F32),
        vm((kv_heads, 1, pair), F32), vm((kv_heads, 1, pair), F32), vm((kv_heads, 1, pair), F32),
        vm((cols, 2) + full, F32), vm((3,) + full, BF16), vm((num_heads, 8, 128), F32),
        vm((cols,) + full, BF16), vm((cols,) + full, BF16), vm(full, BF16), vm(full, BF16),
        vm((2,) + full, BF16), vm((2,) + full, BF16),
        dma((7, kv_heads, cores)), dma((7, kv_heads, cores)), dma((cols, kv_heads)), dma((cols, kv_heads)),
        dma((2, kv_heads)), dma((2, kv_heads)), dma((kv_heads,)), dma((kv_heads,)),
        dma((cols, kv_heads)), dma((cols, kv_heads)), dma((kv_heads,)), dma((kv_heads,)), dma((2, kv_heads)), dma((2, kv_heads)),
    ]
    space = pl.BlockSpec(memory_space=pltpu.VMEM)
    return pl.pallas_call(
        functools.partial(far_attention_kernel, (kv_heads, cores, cols, rows, width)),
        out_shape=[jax.ShapeDtypeStruct((rows, num_heads * width), BF16), jax.ShapeDtypeStruct((rows, num_heads * width), BF16),
                   jax.ShapeDtypeStruct((rows, 2 * kv_heads * width), BF16), jax.ShapeDtypeStruct((num_heads, 8, 128), F32)],
        in_specs=[pl.BlockSpec(memory_space=pltpu.SMEM), space, space, space],
        out_specs=[space] * 4,
        scratch_shapes=scratch,
        compiler_params=pltpu.CompilerParams(collective_id=0, has_side_effects=True, vmem_limit_bytes=67043328),
        name='far_attention',
    )(sinks, q2, kv2, do2)


def rotate_tile(tile, cos, sin, width):
    half = width // 2
    parts = []
    for start in range(0, tile.shape[1], width):
        first, second = tile[:, start:start + half], tile[:, start + half:start + width]
        parts += [first * cos - second * sin, second * cos + first * sin]
    return jnp.concatenate(parts, axis=1)


def near_mask(shape, me):
    key_row = lax.broadcasted_iota(jnp.int32, shape, 0)
    query_row = lax.broadcasted_iota(jnp.int32, shape, 1)
    first_key = jnp.where(me > 0, 0, WINDOW)
    return (key_row >= first_key) & (key_row - WINDOW <= query_row) & (key_row >= query_row)


def forward_kernel(dims, sink_ref, hid_ref, grad_ref, gain_ref, bqkv_ref, bout_ref, cos_ref, sin_ref, wqkv_hbm, wout_hbm,
                   q_one, ext_one, lse_one, mid_out, q_two, kv_two, do_two,
                   ring, wout_one, wout_two, normed, attn, ring_sem, wout_sem, halo_ssem, halo_rsem):
    kv_heads, num_heads, rows, width, model, num_shards, tile, depth = dims
    me = lax.axis_index('cp')
    follow, before = lax.rem(me + 1, num_shards), lax.rem(me + num_shards - 1, num_shards)
    group = num_heads // kv_heads
    qw = num_heads * width
    kw = kv_heads * width
    q_tiles, k_tiles = qw // tile, kw // tile
    per_layer = q_tiles + 2 * k_tiles
    scale = width ** -0.5

    def weight(seq):
        layer, spot = seq // per_layer, lax.rem(seq, per_layer)
        col = pl.multiple_of(lax.rem(spot + q_tiles, per_layer) * tile, tile)
        slot = lax.rem(seq, depth)
        return pltpu.make_async_copy(wqkv_hbm.at[layer, :, pl.ds(col, tile)], ring.at[slot], ring_sem.at[slot])

    for seq in range(depth):
        weight(seq).start()

    barrier = pltpu.get_barrier_semaphore()
    for other in (follow, before):
        pl.semaphore_signal(barrier, inc=1, device_id={'cp': other}, device_id_type=MESH)
    pl.semaphore_wait(barrier, 2)

    def normalize(source, layer):
        def step(r, carry):
            span = pl.ds(pl.multiple_of(r * 16, 16), 16)
            hid = source[span, :].astype(F32)
            inv = lax.rsqrt(jnp.mean(hid * hid, axis=-1, keepdims=True) + EPSILON)
            normed[span, :] = (hid * inv * gain_ref[layer:layer + 1, :]).astype(BF16)
            return carry

        lax.fori_loop(0, rows // 16, step, 0)

    def project(layer, first, count, rotate, store):
        def step(i, carry):
            seq = layer * per_layer + first + i
            weight(seq).wait()
            col = pl.multiple_of((first + q_tiles + i) % per_layer * tile, tile)
            out = jnp.dot(normed[...], ring[lax.rem(seq, depth)], preferred_element_type=F32) + bqkv_ref[layer:layer + 1, pl.ds(col, tile)]
            if rotate:
                out = rotate_tile(out, cos_ref[...], sin_ref[...], width)
            store(i, out.astype(BF16))

            @pl.when(seq + depth < 2 * per_layer)
            def _():
                weight(seq + depth).start()
            return carry

        lax.fori_loop(0, count, step, 0)

    def at(col):
        return pl.ds(pl.multiple_of(col * tile, tile), tile)

    def halo(i):
        return pltpu.make_async_remote_copy(src_ref=ext_one.at[pl.ds(rows, WINDOW), at(i)], dst_ref=ext_one.at[pl.ds(0, WINDOW), at(i)],
                                            send_sem=halo_ssem.at[i], recv_sem=halo_rsem.at[i], device_id={'cp': follow}, device_id_type=MESH)

    def store_near(base):
        def store(i, out):
            ext_one[pl.ds(WINDOW, rows), at(base + i)] = out
            halo(base + i).start()
        return store

    def store_flat(ref, base):
        def store(i, out):
            ref[:, at(base + i)] = out
        return store

    normalize(hid_ref, 0)
    project(0, 0, k_tiles, True, store_near(0))
    project(0, k_tiles, k_tiles, False, store_near(k_tiles))
    load_two = pltpu.make_async_copy(wout_hbm.at[1], wout_two, wout_sem.at[1])
    load_two.start()
    project(0, 2 * k_tiles, q_tiles, True, store_flat(q_one, 0))
    load_one = pltpu.make_async_copy(wout_hbm.at[0], wout_one, wout_sem.at[0])
    load_one.start()

    load_two.wait()

    def attn_grad(i, carry):
        do_two[:, at(i)] = lax.dot_general(grad_ref[...], wout_two[at(i), :], (((1,), (1,)), ((), ())), preferred_element_type=F32).astype(BF16)
        return carry

    lax.fori_loop(0, q_tiles, attn_grad, 0)
    for i in range(2 * k_tiles):
        halo(i).wait_recv()

    def near_head(h, carry):
        kv = h // group
        key_cols = pl.ds(pl.multiple_of(kv * width, width), width)
        value_cols = pl.ds(pl.multiple_of(kw + kv * width, width), width)
        head_cols = pl.ds(pl.multiple_of(h * width, width), width)
        logits = lax.dot_general(ext_one[:, key_cols], q_one[:, head_cols], (((1,), (1,)), ((), ())), preferred_element_type=F32) * scale
        logits = jnp.where(near_mask(logits.shape, me), logits, -jnp.inf)
        sink = sink_ref[0, h]
        peak = jnp.maximum(jnp.max(logits, axis=0, keepdims=True), sink)
        weights = jnp.exp(logits - peak)
        total = jnp.sum(weights, axis=0, keepdims=True) + jnp.exp(sink - peak)
        prob = (weights / total).astype(BF16)
        lse_one[h] = peak + jnp.log(total)
        attn[:, head_cols] = lax.dot_general(prob, ext_one[:, value_cols], (((0,), (0,)), ((), ())), preferred_element_type=F32).astype(BF16)
        return carry

    lax.fori_loop(0, num_heads, near_head, 0)
    load_one.wait()

    def mix(i, carry):
        out = jnp.dot(attn[...], wout_one[:, at(i)], preferred_element_type=F32)
        mid_out[:, at(i)] = (hid_ref[:, at(i)].astype(F32) + (out + bout_ref[0:1, at(i)])).astype(BF16)
        return carry

    lax.fori_loop(0, model // tile, mix, 0)
    normalize(mid_out, 1)
    project(1, 0, k_tiles, True, store_flat(kv_two, 0))
    project(1, k_tiles, k_tiles, False, store_flat(kv_two, k_tiles))
    project(1, 2 * k_tiles, q_tiles, True, store_flat(q_two, 0))
    for i in range(2 * k_tiles):
        halo(i).wait_send()


def backward_kernel(dims, sink_ref, sink_two, o_two, dq_two, dkv_two, hid_ref, mid_ref, grad_ref, q_one, ext_one, lse_one, gain_ref, bout_ref, cos_ref, sin_ref, wqkv_hbm, wout_hbm,
                    out_ref, d_hid_ref, d_gain_ref, d_bqkv_ref, d_bout_ref, d_sink_ref,
                    ring, wout_one, wout_two, d_proj, d_norm, d_mid, d_attn, d_own, halo_send, halo_recv, sums, sink_one, ring_sem, wout_sem, halo_ssem, halo_rsem):
    kv_heads, num_heads, rows, width, model, num_shards, tile, depth = dims
    me = lax.axis_index('cp')
    follow, before = lax.rem(me + 1, num_shards), lax.rem(me + num_shards - 1, num_shards)
    group = num_heads // kv_heads
    qw = num_heads * width
    kw = kv_heads * width
    tiles = model // tile
    scale = width ** -0.5

    def weight(seq):
        layer, spot = 1 - seq // tiles, lax.rem(seq, tiles)
        slot = lax.rem(seq, depth)
        return pltpu.make_async_copy(wqkv_hbm.at[layer, pl.ds(pl.multiple_of(spot * tile, tile), tile), :], ring.at[slot], ring_sem.at[slot])

    for seq in range(depth):
        weight(seq).start()
    load_one = pltpu.make_async_copy(wout_hbm.at[0], wout_one, wout_sem.at[0])
    load_two = pltpu.make_async_copy(wout_hbm.at[1], wout_two, wout_sem.at[1])

    barrier = pltpu.get_barrier_semaphore()
    for other in (follow, before):
        pl.semaphore_signal(barrier, inc=1, device_id={'cp': other}, device_id_type=MESH)
    pl.semaphore_wait(barrier, 2)

    def at(col):
        return pl.ds(pl.multiple_of(col * tile, tile), tile)

    def head_at(h):
        return pl.ds(pl.multiple_of(h * width, width), width)

    def unrotate(layer, h, grad):
        out = rotate_tile(grad.astype(F32), cos_ref[...], -sin_ref[...], width)
        put(layer, h, out)

    def put(layer, h, out):
        d_bqkv_ref[layer:layer + 1, head_at(h)] = jnp.sum(out, axis=0, keepdims=True)
        d_proj[:, head_at(h)] = out.astype(BF16)

    def project_back(layer, source, skip_ref, target):
        def step(i, carry):
            seq = (1 - layer) * tiles + i
            weight(seq).wait()
            out = lax.dot_general(d_proj[...], ring[lax.rem(seq, depth)], (((1,), (1,)), ((), ())), preferred_element_type=F32)
            d_norm[:, at(i)] = out.astype(BF16)

            @pl.when(seq + depth < 2 * tiles)
            def _():
                weight(seq + depth).start()
            return carry

        lax.fori_loop(0, tiles, step, 0)
        sums[...] = jnp.zeros_like(sums)

        def fold(value):
            return value[:8] + value[8:]

        def finish(r, carry):
            span = pl.ds(pl.multiple_of(r * 16, 16), 16)
            hid = source[span, :].astype(F32)
            inv = lax.rsqrt(jnp.mean(hid * hid, axis=-1, keepdims=True) + EPSILON)
            grad = d_norm[span, :].astype(F32)
            sums[0] += fold(grad * hid * inv)
            unit = grad * gain_ref[layer:layer + 1, :]
            d_hid = inv * unit - hid * (inv * inv * inv) * jnp.mean(unit * hid, axis=-1, keepdims=True)
            skip = skip_ref[span, :].astype(F32)
            total = (skip + d_hid).astype(BF16)
            target[span, :] = total
            if layer == 1:
                sums[1] += fold(skip)
                sums[2] += fold(total.astype(F32))
            return carry

        lax.fori_loop(0, rows // 16, finish, 0)
        d_gain_ref[layer:layer + 1, :] = jnp.sum(sums[0], axis=0, keepdims=True)
        if layer == 1:
            d_bout_ref[1:2, :] = jnp.sum(sums[1], axis=0, keepdims=True)
            d_bout_ref[0:1, :] = jnp.sum(sums[2], axis=0, keepdims=True)

    def two_heads(h, carry):
        unrotate(1, h, dq_two[:, head_at(h)])
        return carry

    def two_keys(h, carry):
        unrotate(1, num_heads + h, dkv_two[:, head_at(h)])
        return carry

    def two_values(h, carry):
        put(1, num_heads + kv_heads + h, dkv_two[:, head_at(kv_heads + h)].astype(F32))
        return carry

    lax.fori_loop(0, num_heads, two_heads, 0)
    lax.fori_loop(0, kv_heads, two_keys, 0)
    lax.fori_loop(0, kv_heads, two_values, 0)
    load_one.start()
    project_back(1, mid_ref, grad_ref, d_mid)
    load_two.start()
    load_one.wait()

    def attn_grad(i, carry):
        d_attn[:, at(i)] = lax.dot_general(d_mid[...], wout_one[at(i), :], (((1,), (1,)), ((), ())), preferred_element_type=F32).astype(BF16)
        return carry

    lax.fori_loop(0, qw // tile, attn_grad, 0)

    def halo(g):
        return pltpu.make_async_remote_copy(src_ref=halo_send.at[g], dst_ref=halo_recv.at[g], send_sem=halo_ssem.at[g], recv_sem=halo_rsem.at[g],
                                            device_id={'cp': before}, device_id_type=MESH)

    def near_group(g, carry):
        key_blk, value_blk = ext_one[:, head_at(g)], ext_one[:, head_at(kv_heads + g)]
        d_key = d_value = None
        for part in range(group):
            h = g * group + part
            query_blk, grad_blk = q_one[:, head_at(h)], d_attn[:, head_at(h)]
            logits = lax.dot_general(key_blk, query_blk, (((1,), (1,)), ((), ())), preferred_element_type=F32) * scale
            logits = jnp.where(near_mask(logits.shape, me), logits, -jnp.inf)
            lse = lse_one[h]
            prob = jnp.exp(logits - lse)
            d_prob = lax.dot_general(value_blk, grad_blk, (((1,), (1,)), ((), ())), preferred_element_type=F32).astype(BF16).astype(F32)
            delta = jnp.sum(prob * d_prob, axis=0, keepdims=True)
            d_score = (prob * (d_prob - delta)).astype(BF16)
            d_query = lax.dot_general(d_score, key_blk, (((0,), (0,)), ((), ())), preferred_element_type=F32) * scale
            unrotate(0, h, d_query.astype(BF16))
            d_sink = -jnp.sum(jnp.exp(sink_ref[0, h] - lse) * delta, axis=1, keepdims=True)
            sink_one[h] = jnp.zeros(sink_one.shape[1:], F32) + d_sink
            one_key = jnp.dot(d_score, query_blk, preferred_element_type=F32)
            one_value = jnp.dot(prob.astype(BF16), grad_blk, preferred_element_type=F32)
            d_key = one_key if d_key is None else d_key + one_key
            d_value = one_value if d_value is None else d_value + one_value
        d_key = d_key * scale
        halo_send[g, 0] = d_key[:WINDOW].astype(BF16)
        halo_send[g, 1] = d_value[:WINDOW].astype(BF16)
        d_own[0, g] = d_key[WINDOW:]
        d_own[1, g] = d_value[WINDOW:]
        halo(g).start()
        return carry

    lax.fori_loop(0, kv_heads, near_group, 0)
    load_two.wait()

    def mix(i, carry):
        out = jnp.dot(o_two[...], wout_two[:, at(i)], preferred_element_type=F32)
        out_ref[:, at(i)] = (mid_ref[:, at(i)].astype(F32) + (out + bout_ref[1:2, at(i)])).astype(BF16)
        return carry

    lax.fori_loop(0, tiles, mix, 0)
    for g in range(kv_heads):
        halo(g).wait_recv()
    tail = pl.ds(rows - WINDOW, WINDOW)

    def near_finish(g, carry):
        for kind in range(2):
            d_own[kind, g, tail] += halo_recv[g, kind].astype(F32)
        unrotate(0, num_heads + g, d_own[0, g].astype(BF16))
        put(0, num_heads + kv_heads + g, d_own[1, g].astype(BF16).astype(F32))
        return carry

    lax.fori_loop(0, kv_heads, near_finish, 0)
    lane = lax.broadcasted_iota(jnp.int32, (1, 128), 1)
    for layer, source in ((0, sink_one), (1, sink_two)):
        line = jnp.zeros((1, 128), F32)
        for h in range(num_heads):
            line = jnp.where(lane == h, source[h, 0:1, :], line)
        d_sink_ref[layer:layer + 1, :] = line[:, :num_heads]
    project_back(0, hid_ref, d_mid, d_hid_ref)
    for g in range(kv_heads):
        halo(g).wait_send()


def forward_call(hid, grad, gain, bqkv, bout, cos, sin, wqkv, wout, sinks, kv_heads, num_shards):
    rows, model = hid.shape
    num_heads = sinks.shape[1]
    width = wout.shape[1] // num_heads
    qw, kw = num_heads * width, kv_heads * width
    tile, depth = 512, 4
    vm, dma = pltpu.VMEM, pltpu.SemaphoreType.DMA
    space, far = pl.BlockSpec(memory_space=pltpu.VMEM), pl.BlockSpec(memory_space=pl.ANY)
    shape = jax.ShapeDtypeStruct
    return pl.pallas_call(
        functools.partial(forward_kernel, (kv_heads, num_heads, rows, width, model, num_shards, tile, depth)),
        out_shape=[shape((rows, qw), BF16), shape((WINDOW + rows, 2 * kw), BF16), shape((num_heads, 1, rows), F32), shape((rows, model), BF16),
                   shape((rows, qw), BF16), shape((rows, 2 * kw), BF16), shape((rows, qw), BF16)],
        in_specs=[pl.BlockSpec(memory_space=pltpu.SMEM)] + [space] * 7 + [far] * 2,
        out_specs=[space] * 7,
        scratch_shapes=[vm((depth, model, tile), BF16), vm((qw, model), BF16), vm((qw, model), BF16), vm((rows, model), BF16), vm((rows, qw), BF16),
                        dma((depth,)), dma((2,)), dma((2 * kw // tile,)), dma((2 * kw // tile,))],
        compiler_params=pltpu.CompilerParams(collective_id=1, has_side_effects=True, vmem_limit_bytes=67043328),
        name='forward_dense',
    )(sinks, hid, grad, gain, bqkv, bout, cos, sin, wqkv, wout)


def backward_call(dsink_two, o_two, dq_two, dkv_two, hid, mid, grad, q_one, ext_one, lse_one, gain, bout, cos, sin, wqkv, wout, sinks, kv_heads, num_shards):
    rows, model = hid.shape
    num_heads = sinks.shape[1]
    width = wout.shape[1] // num_heads
    qw, kw = num_heads * width, kv_heads * width
    tile, depth = 512, 3
    vm, dma = pltpu.VMEM, pltpu.SemaphoreType.DMA
    space, far = pl.BlockSpec(memory_space=pltpu.VMEM), pl.BlockSpec(memory_space=pl.ANY)
    shape = jax.ShapeDtypeStruct
    return pl.pallas_call(
        functools.partial(backward_kernel, (kv_heads, num_heads, rows, width, model, num_shards, tile, depth)),
        out_shape=[shape((rows, model), BF16), shape((rows, model), BF16), shape((2, model), F32), shape((2, qw + 2 * kw), F32), shape((2, model), F32),
                   shape((2, num_heads), F32)],
        in_specs=[pl.BlockSpec(memory_space=pltpu.SMEM)] + [space] * 14 + [far] * 2,
        out_specs=[space] * 6,
        scratch_shapes=[vm((depth, tile, qw + 2 * kw), BF16), vm((qw, model), BF16), vm((qw, model), BF16), vm((rows, qw + 2 * kw), BF16), vm((rows, model), BF16),
                        vm((rows, model), BF16), vm((rows, qw), BF16), vm((2, kv_heads, rows, width), F32),
                        vm((kv_heads, 2, WINDOW, width), BF16), vm((kv_heads, 2, WINDOW, width), BF16),
                        vm((3, 8, model), F32), vm((num_heads, 8, 128), F32),
                        dma((depth,)), dma((2,)), dma((kv_heads,)), dma((kv_heads,))],
        compiler_params=pltpu.CompilerParams(collective_id=2, has_side_effects=True, vmem_limit_bytes=67043328),
        name='backward_dense',
    )(sinks, dsink_two, o_two, dq_two, dkv_two, hid, mid, grad, q_one, ext_one, lse_one, gain, bout, cos, sin, wqkv, wout)


def solution(mesh):
    num_shards = mesh.shape['cp']
    row_spec = P('dp', 'cp')
    device_spec = P(('dp', 'cp'))
    whole_spec = P()

    def local_step(hidden, grad_out, norm_gain, w_qkv, b_qkv, w_out, b_out, attn_sinks):
        seq_dev = hidden.shape[1]
        num_heads = attn_sinks.shape[1]
        head_dim = w_out.shape[1] // num_heads
        kv_heads = (w_qkv.shape[2] // head_dim - num_heads) // 2
        row_pos = lax.axis_index('cp') * seq_dev + jnp.arange(seq_dev)
        cos_tab, sin_tab = rope_tables(row_pos, head_dim)
        hid, grad = hidden[0], grad_out[0]

        query_one, near_one, lse_one, middle, query_two, flat_two, d_attn_two = forward_call(
            hid, grad, norm_gain, b_qkv, b_out, cos_tab, sin_tab, w_qkv, w_out, attn_sinks, kv_heads, num_shards)
        attn_two, dq_two, dkv_two, dsink_two = far_attention(query_two, flat_two, d_attn_two, attn_sinks, kv_heads, num_shards)
        output, d_hidden, d_gain, d_bias_qkv, d_bias_out, d_sinks = backward_call(
            dsink_two, attn_two, dq_two, dkv_two, hid, middle, grad, query_one, near_one, lse_one, norm_gain, b_out, cos_tab, sin_tab, w_qkv, w_out, attn_sinks, kv_heads, num_shards)
        return output[None], d_hidden[None], d_gain[None], d_bias_qkv[None], d_bias_out[None], d_sinks[None]

    return jax.shard_map(local_step, mesh=mesh, in_specs=(row_spec, row_spec, whole_spec, whole_spec, whole_spec, whole_spec, whole_spec, whole_spec), out_specs=(row_spec, row_spec, device_spec, device_spec, device_spec, device_spec), check_vma=False)
```

```python
import functools

import jax
import jax.numpy as jnp
import math
from jax import lax
from jax.experimental import pallas as pl
from jax.experimental.pallas import tpu as pltpu
from jax.sharding import PartitionSpec as P

WINDOW = 128
EPSILON = 1e-5
ROPE_THETA = 150000.0
YARN_FACTOR = 32.0
YARN_CONTEXT = 4096.0
YARN_ALPHA = 1.0
YARN_BETA = 32.0


def rope_tables(positions, head_dim):
    half_dim = head_dim // 2
    freq_steps = jnp.arange(half_dim, dtype=jnp.float32)
    freq_base = ROPE_THETA ** (freq_steps * 2.0 / head_dim)
    concentration = 0.1 * math.log(YARN_FACTOR) + 1.0
    low_edge = half_dim * math.log(YARN_CONTEXT / (YARN_BETA * 2.0 * math.pi)) / math.log(ROPE_THETA)
    high_edge = half_dim * math.log(YARN_CONTEXT / (YARN_ALPHA * 2.0 * math.pi)) / math.log(ROPE_THETA)
    ramp_pos = jnp.clip((freq_steps - low_edge) / (high_edge - low_edge), 0.0, 1.0)
    inv_freq = (1.0 - ramp_pos) / freq_base + ramp_pos / (YARN_FACTOR * freq_base)
    angles = positions.astype(jnp.float32)[:, None] * inv_freq[None, :]
    return jnp.cos(angles) * concentration, jnp.sin(angles) * concentration


MESH = pl.DeviceIdType.MESH
F32 = jnp.float32
BF16 = jnp.bfloat16


def far_attention_kernel(dims, sink_ref, q_ref, kv_ref, do_ref, o_out, dq_out, dkv_out, dsink_out,
                         q_all, do_all, kv_all, o_acc, dq_acc, m_ref, l_ref, delta_ref,
                         d_acc, o_stage, ds_stage, sib_send, sib_recv, far_send, far_recv, near_send, near_recv,
                         y_ssem, y_rsem, sib_ssem, sib_rsem, near_ssem, near_rsem, relay_ssem, relay_rsem,
                         bsib_ssem, bsib_rsem, bfar_ssem, bfar_rsem, bnear_ssem, bnear_rsem):
    heads, cores, cols, rows, width = dims
    pair = cores * rows
    scale = width ** -0.5
    me = lax.axis_index('cp')
    core = lax.rem(me, cores)
    x = lax.rem(me // cores, cols)
    y = me // (cores * cols)
    sib = lax.rem(core + 1, cores)

    def device(yy, xx, cc):
        return (yy * cols + xx) * cores + cc

    right = lax.rem(x + 1, cols)
    left = lax.rem(x + cols - 1, cols)
    far = lax.rem(x + 2, cols)
    offsets = [(dy, dc) for dy in (1, 3, 2, 0) for dc in range(cores) if (dy, dc) != (0, 0)]

    barrier = pltpu.get_barrier_semaphore()
    partners = [device(lax.rem(y + dy, heads), x, lax.rem(core + dc, cores)) for dy, dc in offsets]
    partners += [device(y, right, core), device(y, left, core)]
    for other in partners:
        pl.semaphore_signal(barrier, inc=1, device_id={'cp': other}, device_id_type=MESH)
    pl.semaphore_wait(barrier, len(partners))

    def remote(src, dst, ssem, rsem, target):
        return pltpu.make_async_remote_copy(src_ref=src, dst_ref=dst, send_sem=ssem, recv_sem=rsem,
                                            device_id={'cp': target}, device_id_type=MESH)

    pending = []

    def exchange(kind, src_of, dst_of):
        copies = {}
        for dy, dc in offsets + [(0, 0)]:
            ty, tc = lax.rem(y + dy, heads), lax.rem(core + dc, cores)
            if (dy, dc) == (0, 0):
                copy = pltpu.make_async_copy(src_of(ty, tc), dst_of(ty, tc), y_rsem.at[kind, dy, dc])
            else:
                copy = remote(src_of(ty, tc), dst_of(ty, tc), y_ssem.at[kind, dy, dc], y_rsem.at[kind, dy, dc], device(ty, x, tc))
                pending.append(copy)
            copy.start()
            copies[dy, dc] = copy
        return copies

    def arrive(copies, key):
        if key == (0, 0):
            copies[key].wait()
        else:
            copies[key].wait_recv()

    def lanes(block, size):
        return pl.ds(pl.multiple_of(block * size, size), size)

    my_rows = lanes(core, rows)
    kv_copies = exchange(0, lambda ty, tc: kv_ref.at[:, lanes(tc * heads + ty, width)],
                         lambda ty, tc: kv_all.at[tc, x, y, my_rows])
    q_copies = exchange(1, lambda ty, tc: q_ref.at[:, lanes(ty * cores + tc, width)],
                        lambda ty, tc: q_all.at[y, my_rows])
    do_copies = exchange(2, lambda ty, tc: do_ref.at[:, lanes(ty * cores + tc, width)],
                         lambda ty, tc: do_all.at[y, my_rows])

    sink = jnp.minimum(jnp.maximum(sink_ref[1, y * cores + core] * math.log2(math.e), -3.0e38), 3.0e38)
    m_ref[...] = jnp.zeros_like(m_ref) + sink
    l_ref[...] = jnp.ones_like(l_ref)
    o_acc[...] = jnp.zeros_like(o_acc)
    dq_acc[...] = jnp.zeros_like(dq_acc)

    order = (0, 1, 3, 2)
    sib_copies = {}
    near_copies = {}
    relay_copies = {}

    def to_sibling(rel, col, dy, piece):
        copy = remote(kv_all.at[core, col, piece], kv_all.at[core, col, piece], sib_ssem.at[rel, dy], sib_rsem.at[rel, dy], device(y, x, sib))
        copy.start()
        pending.append(copy)
        sib_copies[rel, dy] = copy

    def piece_of(dy):
        return lax.rem(y + heads - dy, heads)

    for dy in order:
        for dc in range(cores):
            arrive(kv_copies, (dy, dc))
        piece = piece_of(dy)
        for way, col in ((0, right), (1, left)):
            copy = remote(kv_all.at[core, x, piece], kv_all.at[core, x, piece], near_ssem.at[way, dy], near_rsem.at[way, dy], device(y, col, core))
            copy.start()
            pending.append(copy)
            near_copies[way, dy] = copy
        to_sibling(0, x, dy, piece)

    def relay(dy):
        piece = piece_of(dy)
        near_copies[0, dy].wait_recv()
        if dy in (0, 1):
            copy = remote(kv_all.at[core, left, piece], kv_all.at[core, left, piece], relay_ssem.at[dy], relay_rsem.at[dy], device(y, right, core))
            copy.start()
            pending.append(copy)
            relay_copies[dy] = copy
        to_sibling(3, left, dy, piece)
        near_copies[1, dy].wait_recv()
        if dy in (2, 3):
            copy = remote(kv_all.at[core, right, piece], kv_all.at[core, right, piece], relay_ssem.at[dy], relay_rsem.at[dy], device(y, left, core))
            copy.start()
            pending.append(copy)
            relay_copies[dy] = copy
        to_sibling(1, right, dy, piece)

    factor = scale * math.log2(math.e)

    def masked_scores(raw, start):
        key_pos = lax.broadcasted_iota(jnp.int32, raw.shape, 0)
        query_pos = lax.broadcasted_iota(jnp.int32, raw.shape, 1) + start
        return jnp.where(key_pos <= query_pos, raw, -jnp.inf)

    def raw_scores(key_blk, yq, masked):
        out = []
        for part in range(cores):
            raw = lax.dot_general(key_blk, q_all[yq, part * rows:(part + 1) * rows], (((1,), (1,)), ((), ())), preferred_element_type=F32)
            out.append(masked_scores(raw, part * rows) if masked else raw)
        return out

    def forward_block(col, yk, queries, masked):
        key_blk, value_blk = kv_all[0, col, yk], kv_all[1, col, yk]
        chains = [(yq, slice(part * rows, (part + 1) * rows)) for yq in queries for part in range(cores)]
        states = [(m_ref[yq, :, span], l_ref[yq, :, span], o_acc[yq, :, span]) for yq, span in chains]
        raws = [raw for yq in queries for raw in raw_scores(key_blk, yq, masked)]
        new = []
        for raw, (old, total, mixed) in zip(raws, states):
            peak = jnp.maximum(old, jnp.max(raw, axis=0, keepdims=True) * factor)
            shrink = jnp.exp2(old - peak)
            weight = jnp.exp2(raw * factor - peak)
            total = total * shrink + jnp.sum(weight, axis=0, keepdims=True)
            mixed = mixed * shrink + lax.dot_general(value_blk, weight.astype(BF16), (((0,), (0,)), ((), ())), preferred_element_type=F32)
            new.append((peak, total, mixed))
        for (yq, span), values in zip(chains, new):
            m_ref[yq, :, span], l_ref[yq, :, span], o_acc[yq, :, span] = values

    def forward_span(col, yk, low):
        count = heads - low
        loop(0, count // 2, lambda n: forward_block(col, yk, (low + 2 * n, low + 2 * n + 1), False))

        @pl.when(lax.rem(count, 2) == 1)
        def _():
            forward_block(col, yk, (heads - 1,), False)

    def backward_block(rel, col, yk, yq, masked):
        key_blk, value_blk = kv_all[0, col, yk], kv_all[1, col, yk]
        lse, delta = m_ref[yq], delta_ref[yq]
        raws = raw_scores(key_blk, yq, masked)
        probs, d_scores = [], []
        for part in range(cores):
            span = slice(part * rows, (part + 1) * rows)
            d_prob = lax.dot_general(value_blk, do_all[yq, span], (((1,), (1,)), ((), ())), preferred_element_type=F32).astype(BF16).astype(F32)
            prob = jnp.exp2(raws[part] * factor - lse[:, span])
            probs.append(prob.astype(BF16))
            d_scores.append((prob * (d_prob - delta[:, span])).astype(BF16))
        prob, d_score = jnp.concatenate(probs, axis=1), jnp.concatenate(d_scores, axis=1)
        d_value = d_acc[rel, 1, yk] + jnp.dot(prob, do_all[yq], preferred_element_type=F32)
        d_key = d_acc[rel, 0, yk] + jnp.dot(d_score, q_all[yq], preferred_element_type=F32)
        d_query = dq_acc[yq] + lax.dot_general(key_blk, d_score, (((0,), (0,)), ((), ())), preferred_element_type=F32)
        d_acc[rel, 1, yk] = d_value
        d_acc[rel, 0, yk] = d_key
        dq_acc[yq] = d_query

    def column(rel):
        return lax.rem(x + rel, cols)

    def loop(low, high, body):
        def step(i, carry):
            body(i)
            return carry
        lax.fori_loop(low, high, step, 0)

    def piece_sweep(block, rel, yk):
        col = column(rel)
        skip = (rel + x) // cols
        loop(yk + 1 - skip, heads, lambda yq: block(col, yk, yq))

    def forward_piece(rel, dy):
        col, piece = column(rel), piece_of(dy)
        remote(kv_all.at[core, col, piece], kv_all.at[core, col, piece], sib_ssem.at[rel, dy], sib_rsem.at[rel, dy], device(y, x, sib)).wait_recv()
        later = 1 - (rel + x) // cols
        forward_span(col, piece, piece + later)

    relay(0)
    relay(1)
    d_acc[...] = jnp.zeros_like(d_acc)
    for key in offsets + [(0, 0)]:
        arrive(q_copies, key)
    for dy in order:
        sib_copies[0, dy].wait_recv()

    def own_forward(yk):
        forward_block(x, yk, (yk,), True)
        forward_span(x, yk, yk + 1)

    loop(0, heads, own_forward)
    relay(3)
    loop(0, 4, lambda j: forward_piece(1 + 2 * lax.rem(j, 2), j // 2))
    relay(2)
    loop(0, 2, lambda j: forward_piece(1 + 2 * j, 3))
    for dy in (0, 1):
        relay_copies[dy].wait_recv()
        to_sibling(2, far, dy, piece_of(dy))
    loop(0, 2, lambda j: forward_piece(1 + 2 * j, 2))
    for dy in (3, 2):
        relay_copies[dy].wait_recv()
        to_sibling(2, far, dy, piece_of(dy))
    loop(0, heads, lambda j: forward_piece(2, j))

    for key in offsets + [(0, 0)]:
        arrive(do_copies, key)

    def finish_forward(yq):
        attn = o_acc[yq] / l_ref[yq]
        lse = m_ref[yq] + jnp.log2(l_ref[yq])
        delta = jnp.sum(attn * jnp.transpose(do_all[yq].astype(F32)), axis=0, keepdims=True)
        o_stage[0, yq] = jnp.transpose(attn).astype(BF16)
        m_ref[yq] = lse
        delta_ref[yq] = delta
        contribution = -jnp.exp2(sink - lse) * delta
        for part in range(cores):
            total = jnp.sum(contribution[:, part * rows:(part + 1) * rows], axis=1, keepdims=True)
            ds_stage[yq * cores + part] = jnp.zeros(ds_stage.shape[1:], F32) + total

    loop(0, heads, finish_forward)

    mine = y * cores + core
    o_copies = exchange(3, lambda ty, tc: o_stage.at[0, ty, lanes(tc, rows)], lambda ty, tc: o_out.at[:, lanes(mine, width)])
    ds_copies = exchange(4, lambda ty, tc: ds_stage.at[ty * cores + tc], lambda ty, tc: dsink_out.at[mine])

    def swap(rel, yk):
        return remote(sib_send.at[rel, yk], sib_recv.at[rel, yk], bsib_ssem.at[rel, yk], bsib_rsem.at[rel, yk], device(y, x, sib))

    def start_swap(rel, yk):
        sib_send[rel, yk] = d_acc[rel, sib, yk].astype(BF16)
        swap(rel, yk).start()

    def chip_total(rel, yk):
        swap(rel, yk).wait_recv()
        return d_acc[rel, core, yk] + sib_recv[rel, yk].astype(F32)

    def backward_piece(rel, yk):
        piece_sweep(lambda col, key, yq: backward_block(rel, col, key, yq, False), rel, yk)

    def far_copy(yk, way):
        target = lax.rem(x + 1 + 2 * way, cols)
        return remote(far_send.at[yk], far_recv.at[yk], bfar_ssem.at[yk], bfar_rsem.at[yk], device(y, target, core))

    def send_far(yk):
        far_send[yk] = chip_total(2, yk).astype(BF16)
        far_copy(yk, lax.rem(yk, 2)).start()

    def far_step(i):
        yk = heads - 1 - i
        backward_piece(2, yk)
        start_swap(2, yk)

        @pl.when(i > 0)
        def _():
            send_far(yk + 1)

    loop(0, heads, far_step)

    def near_key(t):
        side, turn = lax.rem(t, 2), t // 2
        from_left = 2 * lax.rem(turn, 2) + turn // 2
        return 3 - 2 * side, from_left + side * (heads - 1 - 2 * from_left)

    def near_copy(rel, yk):
        return remote(near_send.at[rel // 2, yk], near_recv.at[rel // 2, yk], bnear_ssem.at[rel // 2, yk], bnear_rsem.at[rel // 2, yk], device(y, column(rel), core))

    def send_near(t):
        rel, yk = near_key(t)
        total = chip_total(rel, yk)

        @pl.when(t < heads)
        def _():
            near_send[rel // 2, yk] = total.astype(BF16)

        @pl.when(t >= heads)
        def _():
            far_copy(yk, 0).wait_recv()
            near_send[rel // 2, yk] = (total + far_recv[yk].astype(F32)).astype(BF16)

        near_copy(rel, yk).start()

    def near_step(t):
        rel, yk = near_key(t)
        backward_piece(rel, yk)
        start_swap(rel, yk)

        @pl.when(t == 0)
        def _():
            send_far(0)

        @pl.when(t > 0)
        def _():
            send_near(t - 1)

    loop(0, 2 * heads, near_step)

    def scatter_copy(kind, src, dst, ty, dc):
        tc = lax.rem(core + dc, cores)
        return remote(src.at[ty, lanes(tc, rows)], dst, y_ssem.at[kind, ty, dc], y_rsem.at[kind, y, dc], device(ty, x, tc))

    def scatter(kind, src, dst, ty, act):
        for dc in range(1, cores):
            act(scatter_copy(kind, src, dst, ty, dc))

        @pl.when(ty != y)
        def _():
            act(scatter_copy(kind, src, dst, ty, 0))

    def scatter_wait(kind, src, dst):
        for source in range(heads):
            for dc in range(cores):
                copy = remote(src.at[source, lanes(core, rows)], dst, y_ssem.at[kind, source, dc], y_rsem.at[kind, source, dc], device(y, x, sib))
                if dc == 0:
                    @pl.when(source != y)
                    def _(copy=copy):
                        copy.wait_recv()
                else:
                    copy.wait_recv()
            scatter(kind, src, dst, source, lambda copy: copy.wait_send())

    dq_stage, dkv_stage = o_stage.at[1], o_stage.at[2]
    dq_dst = dq_out.at[:, lanes(mine, width)]
    dkv_dst = dkv_out.at[:, lanes(core * heads + y, width)]

    def own_backward(i):
        yq = heads - 1 - i
        loop(0, yq, lambda yk: backward_block(0, x, yk, yq, False))
        backward_block(0, x, yq, yq, True)
        start_swap(0, yq)

        @pl.when(i == 0)
        def _():
            send_near(2 * heads - 1)
        dq_stage[yq] = jnp.transpose(dq_acc[yq] * scale).astype(BF16)
        scatter(5, dq_stage, dq_dst, yq, lambda copy: copy.start())

    loop(0, heads, own_backward)
    dq_out[:, lanes(mine, width)] = dq_stage[y, lanes(core, rows)]
    key_scale = jnp.where(core == 0, scale, 1.0)

    def own_finish(i):
        yk = lax.rem(i + 1, heads)
        total = chip_total(0, yk)
        for rel in (1, 3):
            near_copy(rel, yk).wait_recv()
            total = total + near_recv[rel // 2, yk].astype(F32)
        dkv_stage[yk] = (total * key_scale).astype(BF16)
        scatter(6, dkv_stage, dkv_dst, yk, lambda copy: copy.start())

    loop(0, heads, own_finish)
    dkv_out[:, lanes(core * heads + y, width)] = dkv_stage[y, lanes(core, rows)]

    for copies in (o_copies, ds_copies):
        for key in offsets + [(0, 0)]:
            arrive(copies, key)
    scatter_wait(5, dq_stage, dq_dst)
    scatter_wait(6, dkv_stage, dkv_dst)

    def drain(yk):
        for rel in range(cols):
            swap(rel, yk).wait_send()
        far_copy(yk, 0).wait_send()
        for rel in (1, 3):
            near_copy(rel, yk).wait_send()

    loop(0, heads, drain)
    for copy in pending:
        copy.wait_send()


def far_attention(q2, kv2, do2, sinks, kv_heads, num_shards):
    rows = q2.shape[0]
    num_heads = sinks.shape[1]
    width = q2.shape[1] // num_heads
    cores = num_heads // kv_heads
    cols = num_shards // num_heads
    assert cols == 4 and kv_heads == 4 and cores == 2
    pair = cores * rows
    full = (kv_heads, pair, width)
    vm, dma = pltpu.VMEM, pltpu.SemaphoreType.DMA
    scratch = [
        vm(full, BF16), vm(full, BF16), vm((2, cols) + full, BF16),
        vm((kv_heads, width, pair), F32), vm((kv_heads, width, pair), F32),
        vm((kv_heads, 1, pair), F32), vm((kv_heads, 1, pair), F32), vm((kv_heads, 1, pair), F32),
        vm((cols, 2) + full, F32), vm((3,) + full, BF16), vm((num_heads, 8, 128), F32),
        vm((cols,) + full, BF16), vm((cols,) + full, BF16), vm(full, BF16), vm(full, BF16),
        vm((2,) + full, BF16), vm((2,) + full, BF16),
        dma((7, kv_heads, cores)), dma((7, kv_heads, cores)), dma((cols, kv_heads)), dma((cols, kv_heads)),
        dma((2, kv_heads)), dma((2, kv_heads)), dma((kv_heads,)), dma((kv_heads,)),
        dma((cols, kv_heads)), dma((cols, kv_heads)), dma((kv_heads,)), dma((kv_heads,)), dma((2, kv_heads)), dma((2, kv_heads)),
    ]
    space = pl.BlockSpec(memory_space=pltpu.VMEM)
    return pl.pallas_call(
        functools.partial(far_attention_kernel, (kv_heads, cores, cols, rows, width)),
        out_shape=[jax.ShapeDtypeStruct((rows, num_heads * width), BF16), jax.ShapeDtypeStruct((rows, num_heads * width), BF16),
                   jax.ShapeDtypeStruct((rows, 2 * kv_heads * width), BF16), jax.ShapeDtypeStruct((num_heads, 8, 128), F32)],
        in_specs=[pl.BlockSpec(memory_space=pltpu.SMEM), space, space, space],
        out_specs=[space] * 4,
        scratch_shapes=scratch,
        compiler_params=pltpu.CompilerParams(collective_id=0, has_side_effects=True, vmem_limit_bytes=67043328),
        name='far_attention',
    )(sinks, q2, kv2, do2)


def rotate_tile(tile, cos, sin, width):
    half = width // 2
    parts = []
    for start in range(0, tile.shape[1], width):
        first, second = tile[:, start:start + half], tile[:, start + half:start + width]
        parts += [first * cos - second * sin, second * cos + first * sin]
    return jnp.concatenate(parts, axis=1)


def near_mask(shape, me):
    key_row = lax.broadcasted_iota(jnp.int32, shape, 0)
    query_row = lax.broadcasted_iota(jnp.int32, shape, 1)
    first_key = jnp.where(me > 0, 0, WINDOW)
    return (key_row >= first_key) & (key_row - WINDOW <= query_row) & (key_row >= query_row)


def forward_kernel(dims, sink_ref, hid_ref, grad_ref, gain_ref, bqkv_ref, bout_ref, cos_ref, sin_ref, wqkv_hbm, wout_hbm,
                   q_one, ext_one, lse_one, mid_out, q_two, kv_two, do_two,
                   ring, wout_one, wout_two, normed, attn, ring_sem, wout_sem, halo_ssem, halo_rsem):
    kv_heads, num_heads, rows, width, model, num_shards, tile, depth = dims
    me = lax.axis_index('cp')
    follow, before = lax.rem(me + 1, num_shards), lax.rem(me + num_shards - 1, num_shards)
    group = num_heads // kv_heads
    qw = num_heads * width
    kw = kv_heads * width
    q_tiles, k_tiles = qw // tile, kw // tile
    per_layer = q_tiles + 2 * k_tiles
    scale = width ** -0.5

    def weight(seq):
        layer, spot = seq // per_layer, lax.rem(seq, per_layer)
        col = pl.multiple_of(lax.rem(spot + q_tiles, per_layer) * tile, tile)
        slot = lax.rem(seq, depth)
        return pltpu.make_async_copy(wqkv_hbm.at[layer, :, pl.ds(col, tile)], ring.at[slot], ring_sem.at[slot])

    for seq in range(depth):
        weight(seq).start()

    barrier = pltpu.get_barrier_semaphore()
    for other in (follow, before):
        pl.semaphore_signal(barrier, inc=1, device_id={'cp': other}, device_id_type=MESH)
    pl.semaphore_wait(barrier, 2)

    def normalize(source, layer):
        hid = source[...].astype(F32)
        inv = lax.rsqrt(jnp.mean(hid * hid, axis=-1, keepdims=True) + EPSILON)
        normed[...] = (hid * inv * gain_ref[layer:layer + 1, :]).astype(BF16)

    def project(layer, first, count, rotate, store):
        def step(i, carry):
            seq = layer * per_layer + first + i
            weight(seq).wait()
            col = pl.multiple_of((first + q_tiles + i) % per_layer * tile, tile)
            out = jnp.dot(normed[...], ring[lax.rem(seq, depth)], preferred_element_type=F32) + bqkv_ref[layer:layer + 1, pl.ds(col, tile)]
            if rotate:
                out = rotate_tile(out, cos_ref[...], sin_ref[...], width)
            store(i, out.astype(BF16))

            @pl.when(seq + depth < 2 * per_layer)
            def _():
                weight(seq + depth).start()
            return carry

        lax.fori_loop(0, count, step, 0, unroll=2)

    def at(col):
        return pl.ds(pl.multiple_of(col * tile, tile), tile)

    def halo(i):
        return pltpu.make_async_remote_copy(src_ref=ext_one.at[pl.ds(rows, WINDOW), at(i)], dst_ref=ext_one.at[pl.ds(0, WINDOW), at(i)],
                                            send_sem=halo_ssem.at[i], recv_sem=halo_rsem.at[i], device_id={'cp': follow}, device_id_type=MESH)

    def store_near(base):
        def store(i, out):
            ext_one[pl.ds(WINDOW, rows), at(base + i)] = out
            halo(base + i).start()
        return store

    def store_flat(ref, base):
        def store(i, out):
            ref[:, at(base + i)] = out
        return store

    normalize(hid_ref, 0)
    project(0, 0, k_tiles, True, store_near(0))
    project(0, k_tiles, k_tiles, False, store_near(k_tiles))
    load_two = pltpu.make_async_copy(wout_hbm.at[1], wout_two, wout_sem.at[1])
    load_two.start()
    project(0, 2 * k_tiles, q_tiles, True, store_flat(q_one, 0))
    load_one = pltpu.make_async_copy(wout_hbm.at[0], wout_one, wout_sem.at[0])
    load_one.start()

    load_two.wait()

    def attn_grad(i, carry):
        do_two[:, at(i)] = lax.dot_general(grad_ref[...], wout_two[at(i), :], (((1,), (1,)), ((), ())), preferred_element_type=F32).astype(BF16)
        return carry

    lax.fori_loop(0, q_tiles, attn_grad, 0, unroll=2)
    for i in range(2 * k_tiles):
        halo(i).wait_recv()

    def near_head(h, carry):
        kv = h // group
        key_cols = pl.ds(pl.multiple_of(kv * width, width), width)
        value_cols = pl.ds(pl.multiple_of(kw + kv * width, width), width)
        head_cols = pl.ds(pl.multiple_of(h * width, width), width)
        logits = lax.dot_general(ext_one[:, key_cols], q_one[:, head_cols], (((1,), (1,)), ((), ())), preferred_element_type=F32) * scale
        logits = jnp.where(near_mask(logits.shape, me), logits, -jnp.inf)
        sink = sink_ref[0, h]
        peak = jnp.maximum(jnp.max(logits, axis=0, keepdims=True), sink)
        weights = jnp.exp(logits - peak)
        total = jnp.sum(weights, axis=0, keepdims=True) + jnp.exp(sink - peak)
        prob = (weights / total).astype(BF16)
        lse_one[h] = peak + jnp.log(total)
        attn[:, head_cols] = lax.dot_general(prob, ext_one[:, value_cols], (((0,), (0,)), ((), ())), preferred_element_type=F32).astype(BF16)
        return carry

    lax.fori_loop(0, num_heads, near_head, 0, unroll=4)
    load_one.wait()

    def mix(i, carry):
        out = jnp.dot(attn[...], wout_one[:, at(i)], preferred_element_type=F32)
        mid_out[:, at(i)] = (hid_ref[:, at(i)].astype(F32) + (out + bout_ref[0:1, at(i)])).astype(BF16)
        return carry

    lax.fori_loop(0, model // tile, mix, 0)
    normalize(mid_out, 1)
    project(1, 0, k_tiles, True, store_flat(kv_two, 0))
    project(1, k_tiles, k_tiles, False, store_flat(kv_two, k_tiles))
    project(1, 2 * k_tiles, q_tiles, True, store_flat(q_two, 0))
    for i in range(2 * k_tiles):
        halo(i).wait_send()


def backward_kernel(dims, sink_ref, sink_two, o_two, dq_two, dkv_two, hid_ref, mid_ref, grad_ref, q_one, ext_one, lse_one, gain_ref, bout_ref, cos_ref, sin_ref, wqkv_hbm, wout_hbm,
                    out_ref, d_hid_ref, d_gain_ref, d_bqkv_ref, d_bout_ref, d_sink_ref,
                    ring, wout_one, wout_two, d_proj, d_norm, d_mid, d_attn, d_own, halo_send, halo_recv, sums, sink_one, ring_sem, wout_sem, halo_ssem, halo_rsem):
    kv_heads, num_heads, rows, width, model, num_shards, tile, depth = dims
    me = lax.axis_index('cp')
    follow, before = lax.rem(me + 1, num_shards), lax.rem(me + num_shards - 1, num_shards)
    group = num_heads // kv_heads
    qw = num_heads * width
    kw = kv_heads * width
    tiles = model // tile
    scale = width ** -0.5

    def weight(seq):
        layer, spot = 1 - seq // tiles, lax.rem(seq, tiles)
        slot = lax.rem(seq, depth)
        return pltpu.make_async_copy(wqkv_hbm.at[layer, pl.ds(pl.multiple_of(spot * tile, tile), tile), :], ring.at[slot], ring_sem.at[slot])

    for seq in range(depth):
        weight(seq).start()
    load_one = pltpu.make_async_copy(wout_hbm.at[0], wout_one, wout_sem.at[0])
    load_two = pltpu.make_async_copy(wout_hbm.at[1], wout_two, wout_sem.at[1])

    barrier = pltpu.get_barrier_semaphore()
    for other in (follow, before):
        pl.semaphore_signal(barrier, inc=1, device_id={'cp': other}, device_id_type=MESH)
    pl.semaphore_wait(barrier, 2)

    def at(col):
        return pl.ds(pl.multiple_of(col * tile, tile), tile)

    def head_at(h):
        return pl.ds(pl.multiple_of(h * width, width), width)

    def unrotate(layer, h, grad):
        out = rotate_tile(grad.astype(F32), cos_ref[...], -sin_ref[...], width)
        put(layer, h, out)

    def put(layer, h, out):
        d_bqkv_ref[layer:layer + 1, head_at(h)] = jnp.sum(out, axis=0, keepdims=True)
        d_proj[:, head_at(h)] = out.astype(BF16)

    def project_back(layer, source, skip_ref, target):
        def step(i, carry):
            seq = (1 - layer) * tiles + i
            weight(seq).wait()
            out = lax.dot_general(d_proj[...], ring[lax.rem(seq, depth)], (((1,), (1,)), ((), ())), preferred_element_type=F32)
            d_norm[:, at(i)] = out.astype(BF16)

            @pl.when(seq + depth < 2 * tiles)
            def _():
                weight(seq + depth).start()
            return carry

        lax.fori_loop(0, tiles, step, 0)
        sums[...] = jnp.zeros_like(sums)

        def fold(value):
            return value[:8] + value[8:]

        def finish(r, carry):
            span = pl.ds(pl.multiple_of(r * 16, 16), 16)
            hid = source[span, :].astype(F32)
            inv = lax.rsqrt(jnp.mean(hid * hid, axis=-1, keepdims=True) + EPSILON)
            grad = d_norm[span, :].astype(F32)
            sums[0] += fold(grad * hid * inv)
            unit = grad * gain_ref[layer:layer + 1, :]
            d_hid = inv * unit - hid * (inv * inv * inv) * jnp.mean(unit * hid, axis=-1, keepdims=True)
            skip = skip_ref[span, :].astype(F32)
            total = (skip + d_hid).astype(BF16)
            target[span, :] = total
            if layer == 1:
                sums[1] += fold(skip)
                sums[2] += fold(total.astype(F32))
            return carry

        lax.fori_loop(0, rows // 16, finish, 0, unroll=2)
        d_gain_ref[layer:layer + 1, :] = jnp.sum(sums[0], axis=0, keepdims=True)
        if layer == 1:
            d_bout_ref[1:2, :] = jnp.sum(sums[1], axis=0, keepdims=True)
            d_bout_ref[0:1, :] = jnp.sum(sums[2], axis=0, keepdims=True)

    def two_heads(h, carry):
        unrotate(1, h, dq_two[:, head_at(h)])
        return carry

    def two_keys(h, carry):
        unrotate(1, num_heads + h, dkv_two[:, head_at(h)])
        return carry

    def two_values(h, carry):
        put(1, num_heads + kv_heads + h, dkv_two[:, head_at(kv_heads + h)].astype(F32))
        return carry

    lax.fori_loop(0, num_heads, two_heads, 0, unroll=4)
    lax.fori_loop(0, kv_heads, two_keys, 0)
    lax.fori_loop(0, kv_heads, two_values, 0)
    load_one.start()
    project_back(1, mid_ref, grad_ref, d_mid)
    load_two.start()
    load_one.wait()

    def attn_grad(i, carry):
        d_attn[:, at(i)] = lax.dot_general(d_mid[...], wout_one[at(i), :], (((1,), (1,)), ((), ())), preferred_element_type=F32).astype(BF16)
        return carry

    lax.fori_loop(0, qw // tile, attn_grad, 0)

    def halo(g):
        return pltpu.make_async_remote_copy(src_ref=halo_send.at[g], dst_ref=halo_recv.at[g], send_sem=halo_ssem.at[g], recv_sem=halo_rsem.at[g],
                                            device_id={'cp': before}, device_id_type=MESH)

    def near_group(g, carry):
        key_blk, value_blk = ext_one[:, head_at(g)], ext_one[:, head_at(kv_heads + g)]
        d_key = d_value = None
        for part in range(group):
            h = g * group + part
            query_blk, grad_blk = q_one[:, head_at(h)], d_attn[:, head_at(h)]
            logits = lax.dot_general(key_blk, query_blk, (((1,), (1,)), ((), ())), preferred_element_type=F32) * scale
            logits = jnp.where(near_mask(logits.shape, me), logits, -jnp.inf)
            lse = lse_one[h]
            prob = jnp.exp(logits - lse)
            d_prob = lax.dot_general(value_blk, grad_blk, (((1,), (1,)), ((), ())), preferred_element_type=F32).astype(BF16).astype(F32)
            delta = jnp.sum(prob * d_prob, axis=0, keepdims=True)
            d_score = (prob * (d_prob - delta)).astype(BF16)
            d_query = lax.dot_general(d_score, key_blk, (((0,), (0,)), ((), ())), preferred_element_type=F32) * scale
            unrotate(0, h, d_query.astype(BF16))
            d_sink = -jnp.sum(jnp.exp(sink_ref[0, h] - lse) * delta, axis=1, keepdims=True)
            sink_one[h] = jnp.zeros(sink_one.shape[1:], F32) + d_sink
            one_key = jnp.dot(d_score, query_blk, preferred_element_type=F32)
            one_value = jnp.dot(prob.astype(BF16), grad_blk, preferred_element_type=F32)
            d_key = one_key if d_key is None else d_key + one_key
            d_value = one_value if d_value is None else d_value + one_value
        d_key = d_key * scale
        halo_send[g, 0] = d_key[:WINDOW].astype(BF16)
        halo_send[g, 1] = d_value[:WINDOW].astype(BF16)
        d_own[0, g] = d_key[WINDOW:]
        d_own[1, g] = d_value[WINDOW:]
        halo(g).start()
        return carry

    lax.fori_loop(0, kv_heads, near_group, 0)
    load_two.wait()

    def mix(i, carry):
        out = jnp.dot(o_two[...], wout_two[:, at(i)], preferred_element_type=F32)
        out_ref[:, at(i)] = (mid_ref[:, at(i)].astype(F32) + (out + bout_ref[1:2, at(i)])).astype(BF16)
        return carry

    lax.fori_loop(0, tiles, mix, 0)
    for g in range(kv_heads):
        halo(g).wait_recv()
    tail = pl.ds(rows - WINDOW, WINDOW)

    def near_finish(g, carry):
        for kind in range(2):
            d_own[kind, g, tail] += halo_recv[g, kind].astype(F32)
        unrotate(0, num_heads + g, d_own[0, g].astype(BF16))
        put(0, num_heads + kv_heads + g, d_own[1, g].astype(BF16).astype(F32))
        return carry

    lax.fori_loop(0, kv_heads, near_finish, 0)
    lane = lax.broadcasted_iota(jnp.int32, (1, 128), 1)
    for layer, source in ((0, sink_one), (1, sink_two)):
        line = jnp.zeros((1, 128), F32)
        for h in range(num_heads):
            line = jnp.where(lane == h, source[h, 0:1, :], line)
        d_sink_ref[layer:layer + 1, :] = line[:, :num_heads]
    project_back(0, hid_ref, d_mid, d_hid_ref)
    for g in range(kv_heads):
        halo(g).wait_send()


def forward_call(hid, grad, gain, bqkv, bout, cos, sin, wqkv, wout, sinks, kv_heads, num_shards):
    rows, model = hid.shape
    num_heads = sinks.shape[1]
    width = wout.shape[1] // num_heads
    qw, kw = num_heads * width, kv_heads * width
    tile, depth = 512, 4
    vm, dma = pltpu.VMEM, pltpu.SemaphoreType.DMA
    space, far = pl.BlockSpec(memory_space=pltpu.VMEM), pl.BlockSpec(memory_space=pl.ANY)
    shape = jax.ShapeDtypeStruct
    return pl.pallas_call(
        functools.partial(forward_kernel, (kv_heads, num_heads, rows, width, model, num_shards, tile, depth)),
        out_shape=[shape((rows, qw), BF16), shape((WINDOW + rows, 2 * kw), BF16), shape((num_heads, 1, rows), F32), shape((rows, model), BF16),
                   shape((rows, qw), BF16), shape((rows, 2 * kw), BF16), shape((rows, qw), BF16)],
        in_specs=[pl.BlockSpec(memory_space=pltpu.SMEM)] + [space] * 7 + [far] * 2,
        out_specs=[space] * 7,
        scratch_shapes=[vm((depth, model, tile), BF16), vm((qw, model), BF16), vm((qw, model), BF16), vm((rows, model), BF16), vm((rows, qw), BF16),
                        dma((depth,)), dma((2,)), dma((2 * kw // tile,)), dma((2 * kw // tile,))],
        compiler_params=pltpu.CompilerParams(collective_id=1, has_side_effects=True, vmem_limit_bytes=67043328),
        name='forward_dense',
    )(sinks, hid, grad, gain, bqkv, bout, cos, sin, wqkv, wout)


def backward_call(dsink_two, o_two, dq_two, dkv_two, hid, mid, grad, q_one, ext_one, lse_one, gain, bout, cos, sin, wqkv, wout, sinks, kv_heads, num_shards):
    rows, model = hid.shape
    num_heads = sinks.shape[1]
    width = wout.shape[1] // num_heads
    qw, kw = num_heads * width, kv_heads * width
    tile, depth = 512, 3
    vm, dma = pltpu.VMEM, pltpu.SemaphoreType.DMA
    space, far = pl.BlockSpec(memory_space=pltpu.VMEM), pl.BlockSpec(memory_space=pl.ANY)
    shape = jax.ShapeDtypeStruct
    return pl.pallas_call(
        functools.partial(backward_kernel, (kv_heads, num_heads, rows, width, model, num_shards, tile, depth)),
        out_shape=[shape((rows, model), BF16), shape((rows, model), BF16), shape((2, model), F32), shape((2, qw + 2 * kw), F32), shape((2, model), F32),
                   shape((2, num_heads), F32)],
        in_specs=[pl.BlockSpec(memory_space=pltpu.SMEM)] + [space] * 14 + [far] * 2,
        out_specs=[space] * 6,
        scratch_shapes=[vm((depth, tile, qw + 2 * kw), BF16), vm((qw, model), BF16), vm((qw, model), BF16), vm((rows, qw + 2 * kw), BF16), vm((rows, model), BF16),
                        vm((rows, model), BF16), vm((rows, qw), BF16), vm((2, kv_heads, rows, width), F32),
                        vm((kv_heads, 2, WINDOW, width), BF16), vm((kv_heads, 2, WINDOW, width), BF16),
                        vm((3, 8, model), F32), vm((num_heads, 8, 128), F32),
                        dma((depth,)), dma((2,)), dma((kv_heads,)), dma((kv_heads,))],
        compiler_params=pltpu.CompilerParams(collective_id=2, has_side_effects=True, vmem_limit_bytes=67043328),
        name='backward_dense',
    )(sinks, dsink_two, o_two, dq_two, dkv_two, hid, mid, grad, q_one, ext_one, lse_one, gain, bout, cos, sin, wqkv, wout)


def solution(mesh):
    num_shards = mesh.shape['cp']
    row_spec = P('dp', 'cp')
    device_spec = P(('dp', 'cp'))
    whole_spec = P()

    def local_step(hidden, grad_out, norm_gain, w_qkv, b_qkv, w_out, b_out, attn_sinks):
        seq_dev = hidden.shape[1]
        num_heads = attn_sinks.shape[1]
        head_dim = w_out.shape[1] // num_heads
        kv_heads = (w_qkv.shape[2] // head_dim - num_heads) // 2
        row_pos = lax.axis_index('cp') * seq_dev + jnp.arange(seq_dev)
        cos_tab, sin_tab = rope_tables(row_pos, head_dim)
        hid, grad = hidden[0], grad_out[0]

        query_one, near_one, lse_one, middle, query_two, flat_two, d_attn_two = forward_call(
            hid, grad, norm_gain, b_qkv, b_out, cos_tab, sin_tab, w_qkv, w_out, attn_sinks, kv_heads, num_shards)
        attn_two, dq_two, dkv_two, dsink_two = far_attention(query_two, flat_two, d_attn_two, attn_sinks, kv_heads, num_shards)
        output, d_hidden, d_gain, d_bias_qkv, d_bias_out, d_sinks = backward_call(
            dsink_two, attn_two, dq_two, dkv_two, hid, middle, grad, query_one, near_one, lse_one, norm_gain, b_out, cos_tab, sin_tab, w_qkv, w_out, attn_sinks, kv_heads, num_shards)
        return output[None], d_hidden[None], d_gain[None], d_bias_qkv[None], d_bias_out[None], d_sinks[None]

    return jax.shard_map(local_step, mesh=mesh, in_specs=(row_spec, row_spec, whole_spec, whole_spec, whole_spec, whole_spec, whole_spec, whole_spec), out_specs=(row_spec, row_spec, device_spec, device_spec, device_spec, device_spec), check_vma=False)
```
